256 devices in a mesh: grp: 2 (over y), seq: 64 (over z, x), head: 2 (over core).
Axes of the slice: x: 4, y: 2, z: 16, core: 2. Of those that a mesh axis runs over, the one named last changes fastest.
The devices are a block of a 4x16x16 slice.
Arguments:
- queries: bfloat16 [1024, 2, 128], P(('grp', 'seq'), 'head'), parts along dimension 0, may hold values from -6 to 6
- keys: bfloat16 [1024, 512, 8, 128], P(('grp', 'seq'), None, 'head'), parts along dimension 0, may hold values from -28 to 28
- values: bfloat16 [1024, 512, 8, 128], P(('grp', 'seq'), None, 'head'), parts along dimension 0, may hold values from -6 to 6
- lengths: int32 [32], P('grp'), parts along dimension 0, may hold values from 1 to 16384, 163840 in all
- slot_block: int32 [1024], P(('grp', 'seq')), parts along dimension 0, may hold values from 0 to 511, each once
Outputs:
- attended: bfloat16 [1024, 2, 128], P(('grp', 'seq'), 'head'), parts along dimension 0
The draws below stay inside these ranges and needn't reach their ends.
There are 2 independent parts, one for each index of `grp`. The reference program is written for one: setup_inputs(seed, part) draws one part's arguments, and reference() takes and returns one part's arrays. A program takes and returns all parts, laid end to end along the dimension named above; each array names one. Nothing has to cross between parts.
Inputs may be any that keep to these rules, and one draw needn't show every extreme that they name: `slot_block`: each slot holds a different logical block; every block of every sequence has a slot. `lengths`: every sequence has at least one token.
All inputs are finite; a program needn't handle non-finite values.
Results may differ from the reference program's by a relative error of at most 0.0055.
Values may be sent and summed in bfloat16 or wider, within the bound.
A program may use at most 64 MiB of HBM per device.

```python
import math
import jax
import jax.numpy as jnp
import numpy as np
from jax import lax

QH = 64
KVH = 8
HD = 128
BLK = 512
BATCH = 16
SLOTS = 512
MAXLEN = 16384
N_HEAD = 2


def draw_queries(key, part):
    base = jnp.clip(jax.random.normal(jax.random.fold_in(key, 21), (BATCH, QH, HD), jnp.float32), -6.0, 6.0)
    base = base.reshape(BATCH, N_HEAD, QH // N_HEAD, HD).transpose(0, 2, 1, 3)
    return base.reshape(BATCH * QH // N_HEAD, N_HEAD, HD).astype(jnp.bfloat16)


def draw_keys(key, part):
    base = jnp.clip(3.0 * jax.random.normal(jax.random.fold_in(key, 31), (SLOTS, BLK, KVH, HD), jnp.float32), -18.0, 18.0)
    return base.astype(jnp.bfloat16)


def steps_of(rng, shape, pieces, low, top_value):
    factor_of = 1.0
    for axis_at, shards_of in pieces:
        draws = jax.random.uniform(jax.random.fold_in(jax.random.fold_in(rng, 6), axis_at), (shards_of,), jnp.float32, low / len(pieces), top_value / len(pieces))
        factor_of = factor_of * jnp.repeat(jnp.exp(draws), shape[axis_at] // shards_of).reshape((-1,) + (1,) * (len(shape) - 1 - axis_at))
    return factor_of


def length_profile(number_of, total, most, lean):
    portions = [(1 << 20) // math.isqrt(rank ** lean) + 1 for rank in range(2, number_of + 1)]
    surplus, counts = total - most - (number_of - 1), [1] * (number_of - 1)
    while surplus > 0:
        candidates = [i for i in range(number_of - 1) if counts[i] < most]
        mass, remaining = sum([portions[i] for i in candidates]), surplus
        for i in candidates:
            more = min(most - counts[i], max(1, remaining * portions[i] // mass), surplus)
            counts[i] = counts[i] + more
            surplus = surplus - more
    return np.array([most] + counts)


def ragged_sizes(key, number_of, total, limit, lean):
    if number_of == 2:
        one = jax.random.randint(key, (), max(1, total - limit), min(limit, total - 1) + 1)
        return jnp.stack([one, total - one])
    sizes = jnp.asarray(length_profile(number_of, total, limit, lean), jnp.int32)
    couples = (number_of - 1) // 2
    giver, taker = sizes[1:1 + 2 * couples:2], sizes[2:2 + 2 * couples:2]
    margin = jnp.minimum(giver - 1, limit - taker)
    passed = jax.random.randint(jax.random.fold_in(key, 1), (couples,), 0, 1 << 20) % (margin + 1)
    sizes = sizes.at[1:1 + 2 * couples:2].set(giver - passed).at[2:2 + 2 * couples:2].set(taker + passed)
    return sizes[jax.random.permutation(jax.random.fold_in(key, 2), number_of)]


def bell_draw(stream_key, extent, width, reach, split=(), held_as=jnp.bfloat16):
    values = jax.random.normal(stream_key, extent, jnp.float32) * width
    if len(split) > 0:
        values = steps_of(stream_key, extent, split, -0.22, 0.18) * values
    return jnp.clip(values, min=-reach, max=reach).astype(held_as)


def setup_inputs(seed: int = 0, part: int = 0) -> dict:
    seeds = jax.random.split(jax.random.key(seed), 6)
    part_splits = jax.random.split(jax.random.fold_in(seeds[5], part), 6)
    queries = draw_queries(jax.random.fold_in(jax.random.fold_in(seeds[5], part), 71), part)
    keys = draw_keys(jax.random.fold_in(jax.random.fold_in(seeds[5], part), 71), part)
    values = bell_draw(part_splits[2], (SLOTS, BLK, KVH, HD), 1.0, 6.0, ((0, 64), (2, 2)))
    lengths = ragged_sizes(part_splits[3], BATCH, 5 * MAXLEN // 8 * BATCH, MAXLEN, 1).astype(jnp.int32)
    slot_block = jax.random.permutation(part_splits[4], SLOTS).astype(jnp.int32)
    return {"queries": queries, "keys": keys, "values": values, "lengths": lengths, "slot_block": slot_block}


def reference(queries, keys, values, lengths, slot_block):
    per_half = QH // N_HEAD
    group = QH // KVH
    per_seq = SLOTS // BATCH
    factor = HD ** -0.5
    q_full = queries.reshape(BATCH, per_half, N_HEAD, HD).transpose(0, 2, 1, 3).reshape(BATCH, KVH, group, HD)

    def one_slot(packed):
        key_blk, val_blk, code = packed
        seq_id = (code // per_seq).astype(jnp.int32)
        blk_id = (code % per_seq).astype(jnp.int32)
        q_one = lax.dynamic_index_in_dim(q_full, seq_id, 0, keepdims=False)
        scores = jnp.einsum('kgd,tkd->kgt', q_one.astype(jnp.float32), key_blk.astype(jnp.float32), precision=lax.Precision.HIGHEST) * factor
        positions = blk_id * BLK + jnp.arange(BLK, dtype=jnp.int32)
        live = (positions < lengths[seq_id])[None, None, :]
        peak = jnp.max(jnp.where(live, scores, -1e30), axis=-1)
        weights = jnp.where(live, jnp.exp(scores - peak[..., None]), 0.0).astype(jnp.bfloat16)
        total = jnp.sum(weights.astype(jnp.float32), axis=-1)
        partial_out = jnp.einsum('kgt,tkd->kgd', weights.astype(jnp.float32), val_blk.astype(jnp.float32), precision=lax.Precision.HIGHEST)
        return peak, total, partial_out

    peaks, totals, partials = lax.map(one_slot, (keys, values, slot_block))
    seq_of = (slot_block // per_seq).astype(jnp.int32)
    member = seq_of[:, None] == jnp.arange(BATCH, dtype=jnp.int32)[None, :]
    best = jnp.max(jnp.where(member[:, :, None, None], peaks[:, None], -1e30), axis=0)
    scaled = jnp.exp(peaks - jnp.take(best, seq_of, axis=0))
    denom = jax.ops.segment_sum(scaled * totals, seq_of, BATCH)
    numer = jax.ops.segment_sum(scaled[..., None] * partials, seq_of, BATCH)
    result = numer / denom[..., None]
    result = result.reshape(BATCH, N_HEAD, per_half, HD).transpose(0, 2, 1, 3).reshape(BATCH * per_half, N_HEAD, HD)
    return result.astype(jnp.bfloat16)
```

```python
import functools
import math

import jax
import jax.numpy as jnp
from jax import lax
from jax.experimental import pallas as pl
from jax.experimental.pallas import tpu as pltpu
from jax.sharding import PartitionSpec as P

MESH = pl.DeviceIdType.MESH
F32 = jnp.float32
BF16 = jnp.bfloat16
NEG = -1e30


def by_distance(count):
    return sorted(range(1, count), key=lambda d: -min(d, count - d)) + [0]


def attend(dims, q_hbm, k_hbm, v_hbm, len_hbm, slot_hbm, o_ref,
           kbuf, vbuf, ktr, q_own, q_all, q_stage, lens, slot, out_send, out_recv, st_send, st_recv,
           ksem, vsem, small_sem, q_send_sem, q_recv_sem, o_send_sem, o_recv_sem, s_send_sem, s_recv_sem):
    nz, nx, slots, block, group, hd = dims
    n = nz * nx
    half = 2
    pairs = nx // half
    rows = half * group
    wide = block * half
    me = lax.axis_index("seq")
    mz, mx = me // nx, lax.rem(me, nx)

    barrier = pltpu.get_barrier_semaphore()
    offsets = [(dz, dx) for dz in by_distance(nz) for dx in by_distance(nx) if dz or dx]
    where = [(lax.rem(mz + dz, nz), lax.rem(mx + dx, nx)) for dz, dx in offsets]
    peers = [z * nx + x for z, x in where]
    for peer in peers:
        pl.semaphore_signal(barrier, inc=1, device_id={"seq": peer}, device_id_type=MESH)

    small = [
        pltpu.make_async_copy(slot_hbm, slot, small_sem.at[0]),
        pltpu.make_async_copy(len_hbm, lens, small_sem.at[1]),
        pltpu.make_async_copy(q_hbm, q_own, small_sem.at[2]),
    ]
    for c in small:
        c.start()
    loads = []
    for s in range(slots):
        kc = pltpu.make_async_copy(k_hbm.at[s], kbuf.at[s], ksem.at[s])
        kc.start()
        loads.append(kc)
    vloads = []
    for s in range(slots):
        vc = pltpu.make_async_copy(v_hbm.at[s], vbuf.at[s], vsem.at[s])
        vc.start()
        vloads.append(vc)
    for c in small:
        c.wait()
    pl.semaphore_wait(barrier, n - 1)

    q_all[me] = q_own[...]
    q_sends = []
    for peer in peers:
        c = pltpu.make_async_remote_copy(
            src_ref=q_own, dst_ref=q_all.at[me], send_sem=q_send_sem, recv_sem=q_recv_sem,
            device_id={"seq": peer}, device_id_type=MESH)
        c.start()

    for s in range(slots):
        loads[s].wait()
        for p in range(pairs):
            ktr[s, p] = kbuf[s, :, p].reshape(wide, hd).T
    for s in range(slots):
        vloads[s].wait()

    rest = q_all.at[pl.ds(0, n - 1)]
    pltpu.make_async_copy(rest, rest, q_recv_sem).wait()

    scale = hd ** -0.5 * math.log2(math.e)
    lane = lax.broadcasted_iota(jnp.int32, (rows, wide), 1)
    row = lax.broadcasted_iota(jnp.int32, (rows, wide), 0)
    matched = lax.rem(lane, half) == row // group
    token = lane // half
    code = [slot[s] for s in range(slots)]
    per_seq = slots * n // nz
    seq = [c // per_seq for c in code]
    left = [lens[b] - lax.rem(c, per_seq) * block for b, c in zip(seq, code)]
    small_lane = lax.broadcasted_iota(jnp.int32, (group, hd), 1)
    small_row = lax.broadcasted_iota(jnp.int32, (group, hd), 0)

    for p in range(pairs):
        peak, total, part = [], [], []
        for s in range(slots):
            q = q_all[pl.ds(seq[s] * nx + p * half, half)].reshape(rows, hd)
            sc = jnp.dot(q, ktr[s, p], preferred_element_type=F32)
            live = matched & (token < left[s])
            sc = jnp.where(live, sc, NEG)
            m = jnp.max(sc, axis=1, keepdims=True)
            w = jnp.where(live, jnp.exp2((sc - m) * scale), 0.0).astype(BF16)
            total.append(jnp.broadcast_to(jnp.sum(w.astype(F32), axis=1, keepdims=True), (rows, hd)))
            part.append(jnp.dot(w, vbuf[s, :, p].reshape(wide, hd), preferred_element_type=F32))
            peak.append(jnp.broadcast_to(m, (rows, hd)))
        for s in range(slots):
            best = peak[s]
            for t in range(slots):
                if t != s:
                    best = jnp.maximum(best, jnp.where(seq[t] == seq[s], peak[t], NEG))
            f = jnp.exp2((peak[s] - best) * scale)
            part[s] = part[s] * f
            total[s] = total[s] * f
        for b in range(nz):
            acc = jnp.zeros((rows, hd), F32)
            den = jnp.zeros((rows, hd), F32)
            top = jnp.full((rows, hd), NEG, F32)
            for s in range(slots):
                mine = seq[s] == b
                acc = acc + jnp.where(mine, part[s], 0.0)
                den = den + jnp.where(mine, total[s], 0.0)
                top = jnp.maximum(top, jnp.where(mine, peak[s], NEG))
            for e in range(half):
                x = p * half + e
                cut = slice(e * group, (e + 1) * group)
                out_send[b, x] = acc[cut].astype(BF16)
                st = jnp.where(small_lane == small_row, top[cut], 0.0)
                st = st + jnp.where(small_lane == small_row + group, den[cut], 0.0)
                st_send[b, x] = jnp.sum(st, axis=0, keepdims=True)
    out_recv[me] = out_send[mz, mx]
    st_recv[me] = st_send[mz, mx]
    for (z, x), peer in zip(where, peers):
        pltpu.make_async_remote_copy(
            src_ref=out_send.at[z, x], dst_ref=out_recv.at[me], send_sem=o_send_sem, recv_sem=o_recv_sem,
            device_id={"seq": peer}, device_id_type=MESH).start()
        pltpu.make_async_remote_copy(
            src_ref=st_send.at[z, x], dst_ref=st_recv.at[me], send_sem=s_send_sem, recv_sem=s_recv_sem,
            device_id={"seq": peer}, device_id_type=MESH).start()

    rest = st_recv.at[pl.ds(0, n - 1)]
    pltpu.make_async_copy(rest, rest, s_recv_sem).wait()
    rest = out_recv.at[pl.ds(0, n - 1)]
    pltpu.make_async_copy(rest, rest, o_recv_sem).wait()

    stat = st_recv[...].reshape(n, hd)
    best = jnp.max(stat, axis=0, keepdims=True)
    f = jnp.exp2((stat - best) * scale)
    den = jnp.sum(f * pltpu.roll(stat, hd - group, 1), axis=0, keepdims=True)
    f = f / den
    acc = jnp.zeros((group, hd), F32)
    for i in range(n):
        g = jnp.where(small_lane == small_row, jnp.broadcast_to(f[i:i + 1], (group, hd)), 0.0)
        g = jnp.sum(g, axis=1, keepdims=True)
        acc = acc + g * out_recv[i].astype(F32)
    o_ref[...] = acc.astype(BF16)

    rest = q_all.at[pl.ds(0, n - 1)]
    pltpu.make_async_copy(rest, rest, q_send_sem).wait()
    rest = out_recv.at[pl.ds(0, n - 1)]
    pltpu.make_async_copy(rest, rest, o_send_sem).wait()
    rest = st_recv.at[pl.ds(0, n - 1)]
    pltpu.make_async_copy(rest, rest, s_send_sem).wait()


def solution(mesh):
    n = mesh.shape["seq"]

    def body(queries, keys, values, lengths, slot_block):
        share, _, hd = queries.shape
        slots, block, kv_local, _ = keys.shape
        nz = lengths.shape[0]
        nx = n // nz
        half = 2
        group = share
        split = (slots, block, nx // half, half, hd)
        any_ = pl.BlockSpec(memory_space=pl.ANY)
        dims = (nz, nx, slots, block, group, hd)
        dma = pltpu.SemaphoreType.DMA
        out = pl.pallas_call(
            functools.partial(attend, dims),
            out_shape=jax.ShapeDtypeStruct((share, hd), BF16),
            in_specs=[any_] * 5,
            out_specs=pl.BlockSpec(memory_space=pltpu.VMEM),
            scratch_shapes=[
                pltpu.VMEM(split, BF16), pltpu.VMEM(split, BF16),
                pltpu.VMEM((slots, nx // half, hd, block * half), BF16),
                pltpu.VMEM((share, hd), BF16), pltpu.VMEM((n, share, hd), BF16), pltpu.VMEM((8, 128), BF16),
                pltpu.SMEM((nz,), jnp.int32), pltpu.SMEM((slots,), jnp.int32),
                pltpu.VMEM((nz, nx, share, hd), BF16), pltpu.VMEM((n, share, hd), BF16),
                pltpu.VMEM((nz, nx, 1, hd), F32), pltpu.VMEM((n, 1, hd), F32),
                dma((slots,)), dma((slots,)), dma((3,)), dma, dma, dma, dma, dma, dma,
            ],
            compiler_params=pltpu.CompilerParams(collective_id=0, has_side_effects=True),
        )(queries.reshape(share, hd), keys.reshape(split), values.reshape(split), lengths, slot_block)
        return out.reshape(share, 1, hd)

    placed = (
        P(("grp", "seq"), "head", None),
        P(("grp", "seq"), None, "head", None),
        P(("grp", "seq"), None, "head", None),
        P("grp"),
        P(("grp", "seq")),
    )
    return jax.shard_map(
        body, mesh=mesh, in_specs=placed, out_specs=P(("grp", "seq"), "head", None), check_vma=False
    )
```

```python
import functools
import math

import jax
import jax.numpy as jnp
from jax import lax
from jax.experimental import pallas as pl
from jax.experimental.pallas import tpu as pltpu
from jax.sharding import PartitionSpec as P

MESH = pl.DeviceIdType.MESH
F32 = jnp.float32
BF16 = jnp.bfloat16
NEG = -1e30


def attend(dims, q_hbm, k_hbm, v_hbm, len_hbm, slot_hbm, o_ref,
           kbuf, vbuf, ktr, q_land, q_use, lens, slot, out_send, out_recv, st_send, st_recv,
           ksem, vsem, small_sem, ready, x_send_sem, x_recv_sem, up_sem, down_sem, block_sem,
           o_send_sem, o_recv_sem, s_send_sem, s_recv_sem):
    nz, nx, slots, block, group, hd = dims
    n = nz * nx
    half = 2
    pairs = nx // half
    rows = half * group
    wide = block * half
    me = lax.axis_index("seq")
    mz, mx = me // nx, lax.rem(me, nx)
    top_z = nz - 1

    def at(z, x):
        return {"seq": z * nx + x}

    barrier = pltpu.get_barrier_semaphore()
    for dx in range(1, nx):
        pl.semaphore_signal(barrier, inc=1, device_id=at(mz, lax.rem(mx + dx, nx)), device_id_type=MESH)

    @pl.when(mz < top_z)
    def _():
        pl.semaphore_signal(barrier, inc=1, device_id=at(mz + 1, mx), device_id_type=MESH)

    small = [
        pltpu.make_async_copy(q_hbm, q_land.at[mz, mx], small_sem.at[2]),
        pltpu.make_async_copy(slot_hbm, slot, small_sem.at[0]),
        pltpu.make_async_copy(len_hbm, lens, small_sem.at[1]),
    ]
    for c in small:
        c.start()
    loads = [pltpu.make_async_copy(k_hbm.at[s], kbuf.at[s], ksem.at[s]) for s in range(slots)]
    vloads = [pltpu.make_async_copy(v_hbm.at[s], vbuf.at[s], vsem.at[s]) for s in range(slots)]
    for c in loads + vloads:
        c.start()
    for c in small:
        c.wait()
    pl.semaphore_wait(barrier, nx - 1 + (mz > 0).astype(jnp.int32))

    @pl.when(mz > 0)
    def _():
        pl.semaphore_signal(ready, inc=1, device_id=at(mz - 1, mx), device_id_type=MESH)

    for dx in range(1, nx):
        pltpu.make_async_remote_copy(
            src_ref=q_land.at[mz, mx], dst_ref=q_land.at[mz, mx], send_sem=x_send_sem, recv_sem=x_recv_sem,
            device_id=at(mz, lax.rem(mx + dx, nx)), device_id_type=MESH).start()
    three = q_land.at[mz, pl.ds(0, nx - 1)]

    def block_copy(b, z, sem):
        return pltpu.make_async_remote_copy(
            src_ref=q_land.at[b], dst_ref=q_land.at[b], send_sem=sem, recv_sem=block_sem.at[b],
            device_id=at(z, mx), device_id_type=MESH)

    def block_wait(b):
        pltpu.make_async_copy(q_land.at[b], q_land.at[b], block_sem.at[b]).wait()

    pltpu.make_async_copy(three, three, x_recv_sem).wait()
    q_use[mz] = q_land[mz]

    @pl.when(mz < top_z)
    def _():
        pl.semaphore_wait(ready, 1)

    for b in range(top_z):
        @pl.when(b < mz)
        def _():
            block_wait(b)

            @pl.when(mz < top_z)
            def _():
                block_copy(b, mz + 1, up_sem.at[b]).start()

            block_copy(mz, b, down_sem.at[b]).start()
            q_use[b] = q_land[b]

    @pl.when(mz < top_z)
    def _():
        block_copy(mz, mz + 1, up_sem.at[mz]).start()

    for s in range(slots):
        loads[s].wait()
        for p in range(pairs):
            ktr[s, p] = kbuf[s, :, p].reshape(wide, hd).T
    for s in range(slots):
        vloads[s].wait()

    scale = hd ** -0.5 * math.log2(math.e)
    per_seq = slots * n // nz
    small_lane = lax.broadcasted_iota(jnp.int32, (group, hd), 1)
    small_row = lax.broadcasted_iota(jnp.int32, (group, hd), 0)

    def one_pass(late, carry):
        @pl.when(late == 1)
        def _():
            for b in range(1, nz):
                @pl.when(b > mz)
                def _():
                    block_wait(b)
                    q_use[b] = q_land[b]

        lane = lax.broadcasted_iota(jnp.int32, (rows, wide), 1)
        row = lax.broadcasted_iota(jnp.int32, (rows, wide), 0)
        matched = lax.rem(lane, half) == row // group
        token = jnp.where(matched, lane // half, block)
        code = [slot[s] for s in range(slots)]
        seq = [c // per_seq for c in code]
        left = []
        for b, c in zip(seq, code):
            rest = jnp.clip(lens[b] - lax.rem(c, per_seq) * block, 0, block)
            ours = (b > mz).astype(jnp.int32) == late
            left.append(jnp.where(ours, rest, 0))
        for p in range(pairs):
            peak, total, part = [], [], []
            for s in range(slots):
                q = q_use[seq[s], pl.ds(p * half, half)].reshape(rows, hd)
                sc = jnp.dot(q, ktr[s, p], preferred_element_type=F32)
                live = token < left[s]
                sc = jnp.where(live, sc, NEG)
                m = jnp.max(sc, axis=1, keepdims=True)
                w = jnp.where(live, jnp.exp2((sc - m) * scale), 0.0).astype(BF16)
                total.append(jnp.broadcast_to(jnp.sum(w.astype(F32), axis=1, keepdims=True), (rows, hd)))
                part.append(jnp.dot(w, vbuf[s, :, p].reshape(wide, hd), preferred_element_type=F32))
                peak.append(jnp.broadcast_to(m, (rows, hd)))
            for s in range(slots):
                best = peak[s]
                for t in range(slots):
                    if t != s:
                        best = jnp.maximum(best, jnp.where(seq[t] == seq[s], peak[t], NEG))
                f = jnp.exp2((peak[s] - best) * scale)
                part[s] = part[s] * f
                total[s] = total[s] * f
            for b in range(nz):
                acc = jnp.zeros((rows, hd), F32)
                den = jnp.zeros((rows, hd), F32)
                top = jnp.full((rows, hd), NEG, F32)
                for s in range(slots):
                    mine = seq[s] == b
                    acc = acc + jnp.where(mine, part[s], 0.0)
                    den = den + jnp.where(mine, total[s], 0.0)
                    top = jnp.maximum(top, jnp.where(mine, peak[s], NEG))
                for e in range(half):
                    x = p * half + e
                    cut = slice(e * group, (e + 1) * group)
                    out_send[late, b, x] = acc[cut].astype(BF16)
                    st = jnp.where(small_lane == small_row, top[cut], 0.0)
                    st = st + jnp.where(small_lane == small_row + group, den[cut], 0.0)
                    st_send[late, b, x] = jnp.sum(st, axis=0, keepdims=True)
            for b in range(nz):
                for e in range(half):
                    x = p * half + e

                    @pl.when(((mz < b).astype(jnp.int32) == late) & (b * nx + x != me))
                    def _():
                        pltpu.make_async_remote_copy(
                            src_ref=out_send.at[late, b, x], dst_ref=out_recv.at[me],
                            send_sem=o_send_sem, recv_sem=o_recv_sem,
                            device_id=at(b, x), device_id_type=MESH).start()
                        pltpu.make_async_remote_copy(
                            src_ref=st_send.at[late, b, x], dst_ref=st_recv.at[me],
                            send_sem=s_send_sem, recv_sem=s_recv_sem,
                            device_id=at(b, x), device_id_type=MESH).start()
        return carry

    lax.fori_loop(0, 2, one_pass, 0)
    out_recv[me] = out_send[0, mz, mx]
    st_recv[me] = st_send[0, mz, mx]

    rest_s = st_recv.at[pl.ds(0, n - 1)]
    rest_o = out_recv.at[pl.ds(0, n - 1)]
    pltpu.make_async_copy(rest_s, rest_s, s_recv_sem).wait()
    pltpu.make_async_copy(rest_o, rest_o, o_recv_sem).wait()

    stat = st_recv[...].reshape(n, hd)
    best = jnp.max(stat, axis=0, keepdims=True)
    f = jnp.exp2((stat - best) * scale)
    den = jnp.sum(f * pltpu.roll(stat, hd - group, 1), axis=0, keepdims=True)
    f = f / den
    acc = jnp.zeros((group, hd), F32)
    for i in range(n):
        g = jnp.where(small_lane == small_row, jnp.broadcast_to(f[i:i + 1], (group, hd)), 0.0)
        g = jnp.sum(g, axis=1, keepdims=True)
        acc = acc + g * out_recv[i].astype(F32)
    o_ref[...] = acc.astype(BF16)

    pltpu.make_async_copy(three, three, x_send_sem).wait()
    for b in range(top_z):
        @pl.when(b < mz)
        def _():
            block_copy(mz, b, down_sem.at[b]).wait_send()

        @pl.when((b <= mz) & (mz < top_z))
        def _():
            block_copy(b, mz + 1, up_sem.at[b]).wait_send()

    pltpu.make_async_copy(rest_o, rest_o, o_send_sem).wait()
    pltpu.make_async_copy(rest_s, rest_s, s_send_sem).wait()


def solution(mesh):
    n = mesh.shape["seq"]

    def body(queries, keys, values, lengths, slot_block):
        share, _, hd = queries.shape
        slots, block, kv_local, _ = keys.shape
        nz = lengths.shape[0]
        nx = n // nz
        half = 2
        group = share
        split = (slots, block, nx // half, half, hd)
        any_ = pl.BlockSpec(memory_space=pl.ANY)
        dims = (nz, nx, slots, block, group, hd)
        dma = pltpu.SemaphoreType.DMA
        out = pl.pallas_call(
            functools.partial(attend, dims),
            out_shape=jax.ShapeDtypeStruct((share, hd), BF16),
            in_specs=[any_] * 5,
            out_specs=pl.BlockSpec(memory_space=pltpu.VMEM),
            scratch_shapes=[
                pltpu.VMEM(split, BF16), pltpu.VMEM(split, BF16),
                pltpu.VMEM((slots, nx // half, hd, block * half), BF16),
                pltpu.VMEM((nz, nx, share, hd), BF16), pltpu.VMEM((nz, nx, share, hd), BF16),
                pltpu.SMEM((nz,), jnp.int32), pltpu.SMEM((slots,), jnp.int32),
                pltpu.VMEM((2, nz, nx, share, hd), BF16), pltpu.VMEM((n, share, hd), BF16),
                pltpu.VMEM((2, nz, nx, 1, hd), F32), pltpu.VMEM((n, 1, hd), F32),
                dma((slots,)), dma((slots,)), dma((3,)), pltpu.SemaphoreType.REGULAR, dma, dma,
                dma((nz,)), dma((nz,)), dma((nz,)), dma, dma, dma, dma,
            ],
            compiler_params=pltpu.CompilerParams(collective_id=0, has_side_effects=True),
        )(queries.reshape(share, hd), keys.reshape(split), values.reshape(split), lengths, slot_block)
        return out.reshape(share, 1, hd)

    placed = (
        P(("grp", "seq"), "head", None),
        P(("grp", "seq"), None, "head", None),
        P(("grp", "seq"), None, "head", None),
        P("grp"),
        P(("grp", "seq")),
    )
    return jax.shard_map(
        body, mesh=mesh, in_specs=placed, out_specs=P(("grp", "seq"), "head", None), check_vma=False
    )
```

```python
import functools
import math

import jax
import jax.numpy as jnp
from jax import lax
from jax.experimental import pallas as pl
from jax.experimental.pallas import tpu as pltpu
from jax.sharding import PartitionSpec as P

MESH = pl.DeviceIdType.MESH
F32 = jnp.float32
BF16 = jnp.bfloat16
NEG = -1e30


def attend(dims, q_hbm, k_hbm, v_hbm, len_hbm, slot_hbm, o_ref,
           kbuf, vbuf, ktr, q_land, q_use, lens, slot, out_send, out_recv, st_send, st_recv,
           ksem, vsem, small_sem, ready, x_ready, x_send_sem, x_recv_sem, block_send, block_sem,
           o_send_sem, o_recv_sem, s_send_sem, s_recv_sem):
    nz, nx, slots, block, group, hd = dims
    n = nz * nx
    half = 2
    pairs = nx // half
    rows = half * group
    wide = block * half
    me = lax.axis_index("seq")
    mz, mx = me // nx, lax.rem(me, nx)
    top_z = nz - 1

    def at(z, x):
        return {"seq": z * nx + x}

    barrier = pltpu.get_barrier_semaphore()
    for z in range(top_z, 0, -1):
        @pl.when(z > mz)
        def _():
            pl.semaphore_signal(barrier, inc=1, device_id=at(z, mx), device_id_type=MESH)

    for x in range(1, nx):
        @pl.when(x > mx)
        def _():
            pl.semaphore_signal(barrier, inc=1, device_id=at(mz, x), device_id_type=MESH)

    small = [
        pltpu.make_async_copy(q_hbm, q_land.at[mz, mx], small_sem.at[2]),
        pltpu.make_async_copy(slot_hbm, slot, small_sem.at[0]),
        pltpu.make_async_copy(len_hbm, lens, small_sem.at[1]),
    ]
    for c in small:
        c.start()
    loads = [pltpu.make_async_copy(k_hbm.at[s], kbuf.at[s], ksem.at[s]) for s in range(slots)]
    vloads = [pltpu.make_async_copy(v_hbm.at[s], vbuf.at[s], vsem.at[s]) for s in range(slots)]
    for c in loads + vloads:
        c.start()
    for c in small:
        c.wait()
    @pl.when(me > 0)
    def _():
        pl.semaphore_wait(barrier, mz + mx)

    for z in range(top_z):
        @pl.when(z < mz)
        def _():
            pl.semaphore_signal(ready.at[mz], inc=1, device_id=at(z, mx), device_id_type=MESH)

    for x in range(nx - 1):
        @pl.when(x < mx)
        def _():
            pl.semaphore_signal(x_ready.at[mx], inc=1, device_id=at(mz, x), device_id_type=MESH)

    for x in range(nx):
        @pl.when(x > mx)
        def _():
            pl.semaphore_wait(x_ready.at[x], 1)

        @pl.when(x != mx)
        def _():
            pltpu.make_async_remote_copy(
                src_ref=q_land.at[mz, mx], dst_ref=q_land.at[mz, mx], send_sem=x_send_sem, recv_sem=x_recv_sem,
                device_id=at(mz, x), device_id_type=MESH).start()
    three = q_land.at[mz, pl.ds(0, nx - 1)]

    def block_copy(b, z, sem):
        return pltpu.make_async_remote_copy(
            src_ref=q_land.at[b], dst_ref=q_land.at[b], send_sem=sem, recv_sem=block_sem.at[b],
            device_id=at(z, mx), device_id_type=MESH)

    def block_wait(b):
        pltpu.make_async_copy(q_land.at[b], q_land.at[b], block_sem.at[b]).wait()

    pltpu.make_async_copy(three, three, x_recv_sem).wait()
    q_use[mz] = q_land[mz]

    for b in range(top_z):
        @pl.when(b < mz)
        def _():
            block_copy(mz, b, block_send.at[b]).start()

    for z in range(1, nz):
        @pl.when(z > mz)
        def _():
            pl.semaphore_wait(ready.at[z], 1)
            block_copy(mz, z, block_send.at[z]).start()

    def first(b):
        d = jnp.abs(mz - b)
        near = jnp.minimum(d, nz - d) <= nz // 4
        return ((b <= mz) & ((mz <= nz // 2) | near)).astype(jnp.int32)

    for s in range(slots):
        loads[s].wait()
        for p in range(pairs):
            ktr[s, p] = kbuf[s, :, p].reshape(wide, hd).T
    for s in range(slots):
        vloads[s].wait()

    scale = hd ** -0.5 * math.log2(math.e)
    per_seq = slots * n // nz
    small_lane = lax.broadcasted_iota(jnp.int32, (group, hd), 1)
    small_row = lax.broadcasted_iota(jnp.int32, (group, hd), 0)

    def one_pass(late, carry):
        for b in range(nz):
            @pl.when((first(b) != late) & (b != mz))
            def _():
                block_wait(b)
                q_use[b] = q_land[b]

        lane = lax.broadcasted_iota(jnp.int32, (rows, wide), 1)
        row = lax.broadcasted_iota(jnp.int32, (rows, wide), 0)
        matched = lax.rem(lane, half) == row // group
        token = jnp.where(matched, lane // half, block)
        code = [slot[s] for s in range(slots)]
        seq = [c // per_seq for c in code]
        left = []
        for b, c in zip(seq, code):
            rest = jnp.clip(lens[b] - lax.rem(c, per_seq) * block, 0, block)
            ours = first(b) != late
            left.append(jnp.where(ours, rest, 0))
        for p in range(pairs):
            peak, total, part = [], [], []
            for s in range(slots):
                q = q_use[seq[s], pl.ds(p * half, half)].reshape(rows, hd)
                sc = jnp.dot(q, ktr[s, p], preferred_element_type=F32)
                live = token < left[s]
                sc = jnp.where(live, sc, NEG)
                m = jnp.max(sc, axis=1, keepdims=True)
                w = jnp.where(live, jnp.exp2((sc - m) * scale), 0.0).astype(BF16)
                total.append(jnp.broadcast_to(jnp.sum(w.astype(F32), axis=1, keepdims=True), (rows, hd)))
                part.append(jnp.dot(w, vbuf[s, :, p].reshape(wide, hd), preferred_element_type=F32))
                peak.append(jnp.broadcast_to(m, (rows, hd)))
            for s in range(slots):
                best = peak[s]
                for t in range(slots):
                    if t != s:
                        best = jnp.maximum(best, jnp.where(seq[t] == seq[s], peak[t], NEG))
                f = jnp.exp2((peak[s] - best) * scale)
                part[s] = part[s] * f
                total[s] = total[s] * f
            for b in range(nz):
                acc = jnp.zeros((rows, hd), F32)
                den = jnp.zeros((rows, hd), F32)
                top = jnp.full((rows, hd), NEG, F32)
                for s in range(slots):
                    mine = seq[s] == b
                    acc = acc + jnp.where(mine, part[s], 0.0)
                    den = den + jnp.where(mine, total[s], 0.0)
                    top = jnp.maximum(top, jnp.where(mine, peak[s], NEG))
                for e in range(half):
                    x = p * half + e
                    cut = slice(e * group, (e + 1) * group)
                    out_send[late, b, x] = acc[cut].astype(BF16)
                    st = jnp.where(small_lane == small_row, top[cut], 0.0)
                    st = st + jnp.where(small_lane == small_row + group, den[cut], 0.0)
                    st_send[late, b, x] = jnp.sum(st, axis=0, keepdims=True)
            for b in range(nz):
                for e in range(half):
                    x = p * half + e

                    @pl.when((first(b) != late) & (b * nx + x != me))
                    def _():
                        pltpu.make_async_remote_copy(
                            src_ref=out_send.at[late, b, x], dst_ref=out_recv.at[me],
                            send_sem=o_send_sem, recv_sem=o_recv_sem,
                            device_id=at(b, x), device_id_type=MESH).start()
                        pltpu.make_async_remote_copy(
                            src_ref=st_send.at[late, b, x], dst_ref=st_recv.at[me],
                            send_sem=s_send_sem, recv_sem=s_recv_sem,
                            device_id=at(b, x), device_id_type=MESH).start()
        return carry

    lax.fori_loop(0, 2, one_pass, 0)
    out_recv[me] = out_send[0, mz, mx]
    st_recv[me] = st_send[0, mz, mx]

    rest_s = st_recv.at[pl.ds(0, n - 1)]
    rest_o = out_recv.at[pl.ds(0, n - 1)]
    pltpu.make_async_copy(rest_s, rest_s, s_recv_sem).wait()
    pltpu.make_async_copy(rest_o, rest_o, o_recv_sem).wait()

    stat = st_recv[...].reshape(n, hd)
    best = jnp.max(stat, axis=0, keepdims=True)
    f = jnp.exp2((stat - best) * scale)
    den = jnp.sum(f * pltpu.roll(stat, hd - group, 1), axis=0, keepdims=True)
    f = f / den
    acc = jnp.zeros((group, hd), F32)
    for i in range(n):
        g = jnp.where(small_lane == small_row, jnp.broadcast_to(f[i:i + 1], (group, hd)), 0.0)
        g = jnp.sum(g, axis=1, keepdims=True)
        acc = acc + g * out_recv[i].astype(F32)
    o_ref[...] = acc.astype(BF16)

    pltpu.make_async_copy(three, three, x_send_sem).wait()
    for z in range(nz):
        @pl.when(z != mz)
        def _():
            block_copy(mz, z, block_send.at[z]).wait_send()

    pltpu.make_async_copy(rest_o, rest_o, o_send_sem).wait()
    pltpu.make_async_copy(rest_s, rest_s, s_send_sem).wait()


def solution(mesh):
    n = mesh.shape["seq"]

    def body(queries, keys, values, lengths, slot_block):
        share, _, hd = queries.shape
        slots, block, kv_local, _ = keys.shape
        nz = lengths.shape[0]
        nx = n // nz
        half = 2
        group = share
        split = (slots, block, nx // half, half, hd)
        any_ = pl.BlockSpec(memory_space=pl.ANY)
        dims = (nz, nx, slots, block, group, hd)
        dma, regular = pltpu.SemaphoreType.DMA, pltpu.SemaphoreType.REGULAR
        out = pl.pallas_call(
            functools.partial(attend, dims),
            out_shape=jax.ShapeDtypeStruct((share, hd), BF16),
            in_specs=[any_] * 5,
            out_specs=pl.BlockSpec(memory_space=pltpu.VMEM),
            scratch_shapes=[
                pltpu.VMEM(split, BF16), pltpu.VMEM(split, BF16),
                pltpu.VMEM((slots, nx // half, hd, block * half), BF16),
                pltpu.VMEM((nz, nx, share, hd), BF16), pltpu.VMEM((nz, nx, share, hd), BF16),
                pltpu.SMEM((nz,), jnp.int32), pltpu.SMEM((slots,), jnp.int32),
                pltpu.VMEM((2, nz, nx, share, hd), BF16), pltpu.VMEM((n, share, hd), BF16),
                pltpu.VMEM((2, nz, nx, 1, hd), F32), pltpu.VMEM((n, 1, hd), F32),
                dma((slots,)), dma((slots,)), dma((3,)), regular((nz,)), regular((nx,)), dma, dma,
                dma((nz,)), dma((nz,)), dma, dma, dma, dma,
            ],
            compiler_params=pltpu.CompilerParams(collective_id=0, has_side_effects=True),
        )(queries.reshape(share, hd), keys.reshape(split), values.reshape(split), lengths, slot_block)
        return out.reshape(share, 1, hd)

    placed = (
        P(("grp", "seq"), "head", None),
        P(("grp", "seq"), None, "head", None),
        P(("grp", "seq"), None, "head", None),
        P("grp"),
        P(("grp", "seq")),
    )
    return jax.shard_map(
        body, mesh=mesh, in_specs=placed, out_specs=P(("grp", "seq"), "head", None), check_vma=False
    )
```

```python
import functools
import math

import jax
import jax.numpy as jnp
from jax import lax
from jax.experimental import pallas as pl
from jax.experimental.pallas import tpu as pltpu
from jax.sharding import PartitionSpec as P

MESH = pl.DeviceIdType.MESH
F32 = jnp.float32
BF16 = jnp.bfloat16
NEG = -1e30


def attend(dims, q_hbm, k_hbm, v_hbm, len_hbm, slot_hbm, o_ref,
           kbuf, vbuf, ktr, gather, gather_stat, q_land, q_use, lens, slot, out_send, out_recv, st_send, st_recv,
           ksem, vsem, small_sem, ready, x_ready, x_send_sem, x_recv_sem, block_send, block_sem,
           o_send_sem, o_recv_sem, s_send_sem, s_recv_sem):
    nz, nx, slots, block, group, hd = dims
    n = nz * nx
    half = 2
    pairs = nx // half
    rows = half * group
    wide = block * half
    me = lax.axis_index("seq")
    mz, mx = me // nx, lax.rem(me, nx)
    top_z = nz - 1

    def at(z, x):
        return {"seq": z * nx + x}

    barrier = pltpu.get_barrier_semaphore()
    for z in range(top_z, 0, -1):
        @pl.when(z > mz)
        def _():
            pl.semaphore_signal(barrier, inc=1, device_id=at(z, mx), device_id_type=MESH)

    for x in range(1, nx):
        @pl.when(x > mx)
        def _():
            pl.semaphore_signal(barrier, inc=1, device_id=at(mz, x), device_id_type=MESH)

    own = pltpu.make_async_copy(q_hbm, q_land.at[mz, mx], small_sem.at[2])
    own.start()

    @pl.when(me > 0)
    def _():
        pl.semaphore_wait(barrier, mz + mx)

    for z in range(top_z):
        @pl.when(z < mz)
        def _():
            pl.semaphore_signal(ready.at[mz], inc=1, device_id=at(z, mx), device_id_type=MESH)

    for x in range(nx - 1):
        @pl.when(x < mx)
        def _():
            pl.semaphore_signal(x_ready.at[mx], inc=1, device_id=at(mz, x), device_id_type=MESH)

    small = [
        pltpu.make_async_copy(slot_hbm, slot, small_sem.at[0]),
        pltpu.make_async_copy(len_hbm, lens, small_sem.at[1]),
    ]
    loads = [pltpu.make_async_copy(k_hbm.at[s], kbuf.at[s], ksem.at[s]) for s in range(slots)]
    vloads = [pltpu.make_async_copy(v_hbm.at[s], vbuf.at[s], vsem.at[s]) for s in range(slots)]
    for c in small + loads + vloads:
        c.start()
    own.wait()
    for x in range(nx):
        @pl.when(x > mx)
        def _():
            pl.semaphore_wait(x_ready.at[x], 1)

        @pl.when(x != mx)
        def _():
            pltpu.make_async_remote_copy(
                src_ref=q_land.at[mz, mx], dst_ref=q_land.at[mz, mx], send_sem=x_send_sem, recv_sem=x_recv_sem,
                device_id=at(mz, x), device_id_type=MESH).start()
    three = q_land.at[mz, pl.ds(0, nx - 1)]

    def block_copy(b, z, sem):
        return pltpu.make_async_remote_copy(
            src_ref=q_land.at[b], dst_ref=q_land.at[b], send_sem=sem, recv_sem=block_sem.at[b],
            device_id=at(z, mx), device_id_type=MESH)

    def block_wait(b):
        pltpu.make_async_copy(q_land.at[b], q_land.at[b], block_sem.at[b]).wait()

    pltpu.make_async_copy(three, three, x_recv_sem).wait()
    q_use[mz] = q_land[mz]

    for b in range(top_z):
        @pl.when(b < mz)
        def _():
            block_copy(mz, b, block_send.at[b]).start()

    for z in range(1, nz):
        @pl.when(z > mz)
        def _():
            pl.semaphore_wait(ready.at[z], 1)
            block_copy(mz, z, block_send.at[z]).start()

    def first(b):
        return (b <= mz).astype(jnp.int32)

    for c in small:
        c.wait()
    per_seq = slots * n // nz
    code = [slot[s] for s in range(slots)]
    seq = [c // per_seq for c in code]
    col = lax.broadcasted_iota(jnp.int32, (1, slots * rows), 1)
    seq_at = jnp.zeros_like(col)
    for s in range(slots):
        seq_at = jnp.where(col // rows == s, seq[s], seq_at)
    r = lax.broadcasted_iota(jnp.int32, (nz * rows, slots * rows), 0)
    c = lax.broadcasted_iota(jnp.int32, (nz * rows, slots * rows), 1)
    gather[...] = jnp.where((r // rows == seq_at) & (lax.rem(r, rows) == lax.rem(c, rows)), 1.0, 0.0).astype(BF16)
    r = lax.broadcasted_iota(jnp.int32, (nz * half, slots * rows), 0)
    c = lax.broadcasted_iota(jnp.int32, (nz * half, slots * rows), 1)
    same = (r // half == seq_at) & (lax.rem(r, half) == lax.rem(c, rows) // group)
    gather_stat[...] = jnp.where(same, 1.0, 0.0).astype(BF16)

    for s in range(slots):
        loads[s].wait()
        for p in range(pairs):
            ktr[s, p] = kbuf[s, :, p].reshape(wide, hd).T
    for s in range(slots):
        vloads[s].wait()

    scale = hd ** -0.5 * math.log2(math.e)
    small_lane = lax.broadcasted_iota(jnp.int32, (group, hd), 1)
    small_row = lax.broadcasted_iota(jnp.int32, (group, hd), 0)

    def one_pass(late, carry):
        for b in range(nz):
            @pl.when((first(b) != late) & (b != mz))
            def _():
                block_wait(b)
                q_use[b] = q_land[b]

        lane = lax.broadcasted_iota(jnp.int32, (rows, wide), 1)
        row = lax.broadcasted_iota(jnp.int32, (rows, wide), 0)
        matched = lax.rem(lane, half) == row // group
        token = jnp.where(matched, lane // half, block)
        left = []
        for b, c in zip(seq, code):
            rest = jnp.clip(lens[b] - lax.rem(c, per_seq) * block, 0, block)
            ours = first(b) != late
            left.append(jnp.where(ours, rest, 0))
        for p in range(pairs):
            peak, total, part = [], [], []
            for s in range(slots):
                q = q_use[seq[s], pl.ds(p * half, half)].reshape(rows, hd)
                sc = jnp.dot(q, ktr[s, p], preferred_element_type=F32)
                live = token < left[s]
                sc = jnp.where(live, sc, NEG)
                m = jnp.max(sc, axis=1, keepdims=True)
                w = jnp.where(live, jnp.exp2((sc - m) * scale), 0.0).astype(BF16)
                total.append(jnp.broadcast_to(jnp.sum(w.astype(F32), axis=1, keepdims=True), (rows, hd)))
                part.append(jnp.dot(w, vbuf[s, :, p].reshape(wide, hd), preferred_element_type=F32))
                peak.append(jnp.broadcast_to(m, (rows, hd)))
            stats = []
            for s in range(slots):
                best = peak[s]
                for t in range(slots):
                    if t != s:
                        best = jnp.maximum(best, jnp.where(seq[t] == seq[s], peak[t], NEG))
                f = jnp.exp2((peak[s] - best) * scale)
                part[s] = part[s] * f
                total[s] = total[s] * f
                head = lax.broadcasted_iota(jnp.int32, (rows, hd), 1) - lax.rem(
                    lax.broadcasted_iota(jnp.int32, (rows, hd), 0), group)
                lead = best
                for t in range(s):
                    lead = jnp.where(seq[t] == seq[s], 0.0, lead)
                stats.append(jnp.where(head == 0, lead, 0.0) + jnp.where(head == group, total[s], 0.0))
            both = jnp.concatenate(part, axis=0).astype(BF16)
            acc = jnp.dot(gather[...], both, preferred_element_type=F32).astype(BF16)
            out_send[late, :, pl.ds(p * half, half)] = acc.reshape(nz, half, group, hd)
            rest = jnp.concatenate(stats, axis=0)
            st = jnp.zeros((nz * half, hd), F32)
            for _ in range(3):
                piece = rest.astype(BF16)
                st = st + jnp.dot(gather_stat[...], piece, preferred_element_type=F32)
                rest = rest - piece.astype(F32)
            st_send[late, :, pl.ds(p * half, half)] = st.reshape(nz, half, 1, hd)
        for b in range(nz):
            @pl.when(first(b) != late)
            def _():
                for x in range(nx):
                    @pl.when(b * nx + x != me)
                    def _():
                        pltpu.make_async_remote_copy(
                            src_ref=out_send.at[late, b, x], dst_ref=out_recv.at[me],
                            send_sem=o_send_sem, recv_sem=o_recv_sem,
                            device_id=at(b, x), device_id_type=MESH).start()
                        pltpu.make_async_remote_copy(
                            src_ref=st_send.at[late, b, x], dst_ref=st_recv.at[me],
                            send_sem=s_send_sem, recv_sem=s_recv_sem,
                            device_id=at(b, x), device_id_type=MESH).start()
        return carry

    lax.fori_loop(0, 1 + (mz < top_z).astype(jnp.int32), one_pass, 0)
    out_recv[me] = out_send[0, mz, mx]
    st_recv[me] = st_send[0, mz, mx]

    rest_s = st_recv.at[pl.ds(0, n - 1)]
    rest_o = out_recv.at[pl.ds(0, n - 1)]
    pltpu.make_async_copy(rest_s, rest_s, s_recv_sem).wait()
    pltpu.make_async_copy(rest_o, rest_o, o_recv_sem).wait()

    stat = st_recv[...].reshape(n, hd)
    total = pltpu.roll(stat, hd - group, 1)
    stat = jnp.where(total > 0.0, stat, NEG)
    best = jnp.max(stat, axis=0, keepdims=True)
    f = jnp.exp2((stat - best) * scale)
    den = jnp.sum(f * total, axis=0, keepdims=True)
    f = f / den
    acc = jnp.zeros((group, hd), F32)
    for i in range(n):
        g = jnp.where(small_lane == small_row, jnp.broadcast_to(f[i:i + 1], (group, hd)), 0.0)
        g = jnp.sum(g, axis=1, keepdims=True)
        acc = acc + g * out_recv[i].astype(F32)
    o_ref[...] = acc.astype(BF16)

    pltpu.make_async_copy(three, three, x_send_sem).wait()
    for z in range(nz):
        @pl.when(z != mz)
        def _():
            block_copy(mz, z, block_send.at[z]).wait_send()

    pltpu.make_async_copy(rest_o, rest_o, o_send_sem).wait()
    pltpu.make_async_copy(rest_s, rest_s, s_send_sem).wait()


def solution(mesh):
    n = mesh.shape["seq"]

    def body(queries, keys, values, lengths, slot_block):
        share, _, hd = queries.shape
        slots, block, kv_local, _ = keys.shape
        nz = lengths.shape[0]
        nx = n // nz
        half = 2
        group = share
        split = (slots, block, nx // half, half, hd)
        any_ = pl.BlockSpec(memory_space=pl.ANY)
        dims = (nz, nx, slots, block, group, hd)
        dma, regular = pltpu.SemaphoreType.DMA, pltpu.SemaphoreType.REGULAR
        out = pl.pallas_call(
            functools.partial(attend, dims),
            out_shape=jax.ShapeDtypeStruct((share, hd), BF16),
            in_specs=[any_] * 5,
            out_specs=pl.BlockSpec(memory_space=pltpu.VMEM),
            scratch_shapes=[
                pltpu.VMEM(split, BF16), pltpu.VMEM(split, BF16),
                pltpu.VMEM((slots, nx // half, hd, block * half), BF16),
                pltpu.VMEM((nz * half * share, slots * half * share), BF16),
                pltpu.VMEM((nz * half, slots * half * share), BF16),
                pltpu.VMEM((nz, nx, share, hd), BF16), pltpu.VMEM((nz, nx, share, hd), BF16),
                pltpu.SMEM((nz,), jnp.int32), pltpu.SMEM((slots,), jnp.int32),
                pltpu.VMEM((2, nz, nx, share, hd), BF16), pltpu.VMEM((n, share, hd), BF16),
                pltpu.VMEM((2, nz, nx, 1, hd), F32), pltpu.VMEM((n, 1, hd), F32),
                dma((slots,)), dma((slots,)), dma((3,)), regular((nz,)), regular((nx,)), dma, dma,
                dma((nz,)), dma((nz,)), dma, dma, dma, dma,
            ],
            compiler_params=pltpu.CompilerParams(collective_id=0, has_side_effects=True),
        )(queries.reshape(share, hd), keys.reshape(split), values.reshape(split), lengths, slot_block)
        return out.reshape(share, 1, hd)

    placed = (
        P(("grp", "seq"), "head", None),
        P(("grp", "seq"), None, "head", None),
        P(("grp", "seq"), None, "head", None),
        P("grp"),
        P(("grp", "seq")),
    )
    return jax.shard_map(
        body, mesh=mesh, in_specs=placed, out_specs=P(("grp", "seq"), "head", None), check_vma=False
    )
```

```python
import functools
import math

import jax
import jax.numpy as jnp
from jax import lax
from jax.experimental import pallas as pl
from jax.experimental.pallas import tpu as pltpu
from jax.sharding import PartitionSpec as P

MESH = pl.DeviceIdType.MESH
F32 = jnp.float32
BF16 = jnp.bfloat16
NEG = -1e30


def attend(dims, q_hbm, k_hbm, v_hbm, len_hbm, slot_hbm, o_ref,
           kbuf, vbuf, ktr, gather, gather_stat, q_land, q_use, lens, slot, out_send, out_recv, st_send, st_recv, z_send, z_recv, zs_send, zs_recv,
           ksem, vsem, small_sem, ready, x_ready, x_send_sem, x_recv_sem, block_send, block_sem,
           relay_send, o_send_sem, o_recv_sem, s_send_sem, s_recv_sem, z_send_sem, z_recv_sem, zs_send_sem, zs_recv_sem):
    nz, nx, slots, block, group, hd = dims
    n = nz * nx
    half = 2
    pairs = nx // half
    rows = half * group
    wide = block * half
    me = lax.axis_index("seq")
    mz, mx = me // nx, lax.rem(me, nx)
    top_z = nz - 1

    reach = nz // 4

    def at(z, x):
        return {"seq": z * nx + x}

    def direct(later, earlier):
        d = later - earlier
        return (d <= reach) | (d >= nz - reach)

    def relayed(b):
        return (mz + reach < nz) & (b < mz) & (b > mz - (nz // 2))

    barrier = pltpu.get_barrier_semaphore()
    for z in range(top_z, 0, -1):
        @pl.when(z > mz)
        def _():
            pl.semaphore_signal(barrier, inc=1, device_id=at(z, mx), device_id_type=MESH)

    for x in range(1, nx):
        @pl.when(x > mx)
        def _():
            pl.semaphore_signal(barrier, inc=1, device_id=at(mz, x), device_id_type=MESH)

    own = pltpu.make_async_copy(q_hbm, q_land.at[mz, mx], small_sem.at[2])
    own.start()

    @pl.when(me > 0)
    def _():
        pl.semaphore_wait(barrier, mz + mx)

    for z in range(top_z):
        @pl.when((z < mz) & direct(mz, z))
        def _():
            pl.semaphore_signal(ready.at[mz], inc=1, device_id=at(z, mx), device_id_type=MESH)

    for x in range(nx - 1):
        @pl.when(x < mx)
        def _():
            pl.semaphore_signal(x_ready.at[mx], inc=1, device_id=at(mz, x), device_id_type=MESH)

    small = [
        pltpu.make_async_copy(slot_hbm, slot, small_sem.at[0]),
        pltpu.make_async_copy(len_hbm, lens, small_sem.at[1]),
    ]
    loads = [pltpu.make_async_copy(k_hbm.at[s], kbuf.at[s], ksem.at[s]) for s in range(slots)]
    vloads = [pltpu.make_async_copy(v_hbm.at[s], vbuf.at[s], vsem.at[s]) for s in range(slots)]
    for c in small + loads + vloads:
        c.start()
    own.wait()
    for x in range(nx):
        @pl.when(x > mx)
        def _():
            pl.semaphore_wait(x_ready.at[x], 1)

        @pl.when(x != mx)
        def _():
            pltpu.make_async_remote_copy(
                src_ref=q_land.at[mz, mx], dst_ref=q_land.at[mz, mx], send_sem=x_send_sem, recv_sem=x_recv_sem,
                device_id=at(mz, x), device_id_type=MESH).start()
    three = q_land.at[mz, pl.ds(0, nx - 1)]

    def block_copy(b, z, sem):
        return pltpu.make_async_remote_copy(
            src_ref=q_land.at[b], dst_ref=q_land.at[b], send_sem=sem, recv_sem=block_sem.at[b],
            device_id=at(z, mx), device_id_type=MESH)

    def block_wait(b):
        pltpu.make_async_copy(q_land.at[b], q_land.at[b], block_sem.at[b]).wait()

    pltpu.make_async_copy(three, three, x_recv_sem).wait()
    q_use[mz] = q_land[mz]

    for b in range(top_z):
        @pl.when(b < mz)
        def _():
            block_copy(mz, b, block_send.at[b]).start()

    for z in range(1, nz):
        @pl.when((z > mz) & direct(z, mz))
        def _():
            pl.semaphore_wait(ready.at[z], 1)
            block_copy(mz, z, block_send.at[z]).start()

        if z > reach:
            @pl.when(z == mz + reach)
            def _():
                for b in range(max(0, z - reach - nz // 2 + 1), z - reach):
                    block_wait(b)
                    block_copy(b, z, relay_send.at[b]).start()

    def first(b):
        return (b <= mz).astype(jnp.int32)

    for c in small:
        c.wait()
    per_seq = slots * n // nz
    code = [slot[s] for s in range(slots)]
    seq = [c // per_seq for c in code]
    col = lax.broadcasted_iota(jnp.int32, (1, slots * rows), 1)
    seq_at = jnp.zeros_like(col)
    for s in range(slots):
        seq_at = jnp.where(col // rows == s, seq[s], seq_at)
    r = lax.broadcasted_iota(jnp.int32, (nz * rows, slots * rows), 0)
    c = lax.broadcasted_iota(jnp.int32, (nz * rows, slots * rows), 1)
    wanted = r // (nz * group) * group + lax.rem(r, group)
    same = (lax.rem(r, nz * group) // group == seq_at) & (wanted == lax.rem(c, rows))
    gather[...] = jnp.where(same, 1.0, 0.0).astype(BF16)
    r = lax.broadcasted_iota(jnp.int32, (nz * half, slots * rows), 0)
    c = lax.broadcasted_iota(jnp.int32, (nz * half, slots * rows), 1)
    same = (lax.rem(r, nz) == seq_at) & (r // nz == lax.rem(c, rows) // group)
    gather_stat[...] = jnp.where(same, 1.0, 0.0).astype(BF16)

    for s in range(slots):
        loads[s].wait()
        for p in range(pairs):
            ktr[s, p] = kbuf[s, :, p].reshape(wide, hd).T
    for s in range(slots):
        vloads[s].wait()

    scale = hd ** -0.5 * math.log2(math.e)

    def to_rows(f):
        r = lax.broadcasted_iota(jnp.int32, (nz * group, hd), 0)
        c = lax.broadcasted_iota(jnp.int32, (nz * group, hd), 1)
        spread = jnp.broadcast_to(f[:, None, :], (nz, group, hd)).reshape(nz * group, hd)
        return jnp.sum(jnp.where(lax.rem(r, group) == c, spread, 0.0), axis=1, keepdims=True)

    def one_pass(late, carry):
        for b in range(nz):
            @pl.when((first(b) != late) & (b != mz) & ~relayed(b))
            def _():
                block_wait(b)

            @pl.when((first(b) != late) & (b != mz))
            def _():
                q_use[b] = q_land[b]

        lane = lax.broadcasted_iota(jnp.int32, (rows, wide), 1)
        row = lax.broadcasted_iota(jnp.int32, (rows, wide), 0)
        matched = lax.rem(lane, half) == row // group
        token = jnp.where(matched, lane // half, block)
        left = []
        for b, c in zip(seq, code):
            rest = jnp.clip(lens[b] - lax.rem(c, per_seq) * block, 0, block)
            ours = first(b) != late
            left.append(jnp.where(ours, rest, 0))
        for p in range(pairs):
            peak, total, part = [], [], []
            for s in range(slots):
                q = q_use[seq[s], pl.ds(p * half, half)].reshape(rows, hd)
                sc = jnp.dot(q, ktr[s, p], preferred_element_type=F32)
                live = token < left[s]
                sc = jnp.where(live, sc, NEG)
                m = jnp.max(sc, axis=1, keepdims=True)
                w = jnp.where(live, jnp.exp2((sc - m) * scale), 0.0).astype(BF16)
                total.append(jnp.broadcast_to(jnp.sum(w.astype(F32), axis=1, keepdims=True), (rows, hd)))
                part.append(jnp.dot(w, vbuf[s, :, p].reshape(wide, hd), preferred_element_type=F32))
                peak.append(jnp.broadcast_to(m, (rows, hd)))
            stats = []
            for s in range(slots):
                best = peak[s]
                for t in range(slots):
                    if t != s:
                        best = jnp.maximum(best, jnp.where(seq[t] == seq[s], peak[t], NEG))
                f = jnp.exp2((peak[s] - best) * scale)
                part[s] = part[s] * f
                total[s] = total[s] * f
                head = lax.broadcasted_iota(jnp.int32, (rows, hd), 1) - lax.rem(
                    lax.broadcasted_iota(jnp.int32, (rows, hd), 0), group)
                lead = best
                for t in range(s):
                    lead = jnp.where(seq[t] == seq[s], 0.0, lead)
                stats.append(jnp.where(head == 0, lead, 0.0) + jnp.where(head == group, total[s], 0.0))
            both = jnp.concatenate(part, axis=0).astype(BF16)
            acc = jnp.dot(gather[...], both, preferred_element_type=F32).astype(BF16)
            for e in range(half):
                out_send[late, p * half + e] = acc[e * nz * group:(e + 1) * nz * group]
            rest = jnp.concatenate(stats, axis=0)
            st = jnp.zeros((nz * half, hd), F32)
            for _ in range(3):
                piece = rest.astype(BF16)
                st = st + jnp.dot(gather_stat[...], piece, preferred_element_type=F32)
                rest = rest - piece.astype(F32)
            for e in range(half):
                st_send[late, p * half + e] = st[e * nz:(e + 1) * nz]
        for x in range(nx):
            @pl.when(x != mx)
            def _():
                pltpu.make_async_remote_copy(
                    src_ref=out_send.at[late, x], dst_ref=out_recv.at[late, mx],
                    send_sem=o_send_sem.at[late], recv_sem=o_recv_sem.at[late],
                    device_id=at(mz, x), device_id_type=MESH).start()
                pltpu.make_async_remote_copy(
                    src_ref=st_send.at[late, x], dst_ref=st_recv.at[late, mx],
                    send_sem=s_send_sem.at[late], recv_sem=s_recv_sem.at[late],
                    device_id=at(mz, x), device_id_type=MESH).start()
        out_recv[late, mx] = out_send[late, mx]
        st_recv[late, mx] = st_send[late, mx]
        peers_o = out_recv.at[late, pl.ds(0, nx - 1)]
        peers_s = st_recv.at[late, pl.ds(0, nx - 1)]
        pltpu.make_async_copy(peers_s, peers_s, s_recv_sem.at[late]).wait()
        pltpu.make_async_copy(peers_o, peers_o, o_recv_sem.at[late]).wait()

        stat = [st_recv[late, x] for x in range(nx)]
        total = [pltpu.roll(v, hd - group, 1) for v in stat]
        stat = [jnp.where(t > 0.0, v, NEG) for v, t in zip(stat, total)]
        best = functools.reduce(jnp.maximum, stat)
        f = [jnp.exp2((v - best) * scale) for v in stat]
        den = sum(g * t for g, t in zip(f, total))
        acc = sum(to_rows(f[x]) * out_recv[late, x].astype(F32) for x in range(nx))
        z_send[late] = acc.reshape(nz, group, hd)
        lane = lax.broadcasted_iota(jnp.int32, (nz, hd), 1)
        both = jnp.where(lane < group, best, jnp.where(lane < 2 * group, pltpu.roll(den, group, 1), 0.0))
        zs_send[late] = both.reshape(nz, 1, hd)
        for b in range(nz):
            @pl.when((first(b) != late) & (b != mz))
            def _():
                pltpu.make_async_remote_copy(
                    src_ref=z_send.at[late, b], dst_ref=z_recv.at[mz], send_sem=z_send_sem, recv_sem=z_recv_sem,
                    device_id=at(b, mx), device_id_type=MESH).start()
                pltpu.make_async_remote_copy(
                    src_ref=zs_send.at[late, b], dst_ref=zs_recv.at[mz], send_sem=zs_send_sem, recv_sem=zs_recv_sem,
                    device_id=at(b, mx), device_id_type=MESH).start()

        pltpu.make_async_copy(peers_s, peers_s, s_send_sem.at[late]).wait()
        pltpu.make_async_copy(peers_o, peers_o, o_send_sem.at[late]).wait()
        return carry

    lax.fori_loop(0, 1 + (mz < top_z).astype(jnp.int32), one_pass, 0)
    z_recv[mz] = z_send[0, mz]
    zs_recv[mz] = zs_send[0, mz]
    rest_s = zs_recv.at[pl.ds(0, nz - 1)]
    rest_z = z_recv.at[pl.ds(0, nz - 1)]
    pltpu.make_async_copy(rest_s, rest_s, zs_recv_sem).wait()
    pltpu.make_async_copy(rest_z, rest_z, z_recv_sem).wait()

    stat = zs_recv[...].reshape(nz, hd)
    total = pltpu.roll(stat, hd - group, 1)
    stat = jnp.where(total > 0.0, stat, NEG)
    best = jnp.max(stat, axis=0, keepdims=True)
    f = jnp.exp2((stat - best) * scale)
    f = f / jnp.sum(f * total, axis=0, keepdims=True)
    acc = to_rows(f) * z_recv[...].reshape(nz * group, hd)
    o_ref[...] = jnp.sum(acc.reshape(nz, group, hd), axis=0).astype(BF16)

    pltpu.make_async_copy(three, three, x_send_sem).wait()
    for z in range(nz):
        @pl.when((z != mz) & ((z < mz) | direct(z, mz)))
        def _():
            block_copy(mz, z, block_send.at[z]).wait_send()

        @pl.when(relayed(z))
        def _():
            block_copy(z, mz + reach, relay_send.at[z]).wait_send()

    pltpu.make_async_copy(rest_z, rest_z, z_send_sem).wait()
    pltpu.make_async_copy(rest_s, rest_s, zs_send_sem).wait()


def solution(mesh):
    n = mesh.shape["seq"]

    def body(queries, keys, values, lengths, slot_block):
        share, _, hd = queries.shape
        slots, block, kv_local, _ = keys.shape
        nz = lengths.shape[0]
        nx = n // nz
        half = 2
        group = share
        split = (slots, block, nx // half, half, hd)
        any_ = pl.BlockSpec(memory_space=pl.ANY)
        dims = (nz, nx, slots, block, group, hd)
        dma, regular = pltpu.SemaphoreType.DMA, pltpu.SemaphoreType.REGULAR
        out = pl.pallas_call(
            functools.partial(attend, dims),
            out_shape=jax.ShapeDtypeStruct((share, hd), BF16),
            in_specs=[any_] * 5,
            out_specs=pl.BlockSpec(memory_space=pltpu.VMEM),
            scratch_shapes=[
                pltpu.VMEM(split, BF16), pltpu.VMEM(split, BF16),
                pltpu.VMEM((slots, nx // half, hd, block * half), BF16),
                pltpu.VMEM((nz * half * share, slots * half * share), BF16),
                pltpu.VMEM((nz * half, slots * half * share), BF16),
                pltpu.VMEM((nz, nx, share, hd), BF16), pltpu.VMEM((nz, nx, share, hd), BF16),
                pltpu.SMEM((nz,), jnp.int32), pltpu.SMEM((slots,), jnp.int32),
                pltpu.VMEM((2, nx, nz * share, hd), BF16), pltpu.VMEM((2, nx, nz * share, hd), BF16),
                pltpu.VMEM((2, nx, nz, hd), F32), pltpu.VMEM((2, nx, nz, hd), F32),
                pltpu.VMEM((2, nz, share, hd), F32), pltpu.VMEM((nz, share, hd), F32),
                pltpu.VMEM((2, nz, 1, hd), F32), pltpu.VMEM((nz, 1, hd), F32),
                dma((slots,)), dma((slots,)), dma((3,)), regular((nz,)), regular((nx,)), dma, dma,
                dma((nz,)), dma((nz,)), dma((nz,)), dma((2,)), dma((2,)), dma((2,)), dma((2,)), dma, dma, dma, dma,
            ],
            compiler_params=pltpu.CompilerParams(collective_id=0, has_side_effects=True),
        )(queries.reshape(share, hd), keys.reshape(split), values.reshape(split), lengths, slot_block)
        return out.reshape(share, 1, hd)

    placed = (
        P(("grp", "seq"), "head", None),
        P(("grp", "seq"), None, "head", None),
        P(("grp", "seq"), None, "head", None),
        P("grp"),
        P(("grp", "seq")),
    )
    return jax.shard_map(
        body, mesh=mesh, in_specs=placed, out_specs=P(("grp", "seq"), "head", None), check_vma=False
    )
```

```python
import functools
import math

import jax
import jax.numpy as jnp
from jax import lax
from jax.experimental import pallas as pl
from jax.experimental.pallas import tpu as pltpu
from jax.sharding import PartitionSpec as P

MESH = pl.DeviceIdType.MESH
F32 = jnp.float32
BF16 = jnp.bfloat16
NEG = -1e30


def attend(dims, q_hbm, k_hbm, v_hbm, len_hbm, slot_hbm, o_ref,
           kbuf, vbuf, ktr, gather, gather_stat, q_land, q_use, lens, slot, out_send, out_recv, st_send, st_recv, z_send, z_recv, zs_send, zs_recv,
           ksem, vsem, small_sem, ready, ready_low, x_ready, root_sem, row_send, row_send_low, root_send, col_send, x_send_sem, x_recv_sem, block_send, block_sem,
           relay_send, o_send_sem, o_recv_sem, s_send_sem, s_recv_sem, z_send_sem, z_recv_sem, zs_send_sem, zs_recv_sem):
    nz, nx, slots, block, group, hd = dims
    n = nz * nx
    half = 2
    pairs = nx // half
    rows = half * group
    wide = block * half
    me = lax.axis_index("seq")
    mz, mx = me // nx, lax.rem(me, nx)
    top_z = nz - 1

    reach = nz // 4

    def at(z, x):
        return {"seq": z * nx + x}

    def direct(later, earlier):
        d = later - earlier
        return (d <= reach) | (d >= nz - reach)

    def relayed(b):
        return (mz + reach < nz) & (b < mz) & (b > mz - (nz // 2))

    low = mz == 0
    root = me == 0
    agent = me == 1

    barrier = pltpu.get_barrier_semaphore()

    def greet(z, x):
        pl.semaphore_signal(barrier, inc=1, device_id=at(z, x), device_id_type=MESH)

    for z in range(top_z, 0, -1):
        @pl.when((z > mz) & ~root)
        def _():
            greet(z, mx)

        @pl.when(agent)
        def _():
            greet(z, 0)

    for x in range(nx):
        @pl.when(((x > mx) & ~root) | ((x == 0) & low & ~root))
        def _():
            greet(mz, x)

    own = pltpu.make_async_copy(q_hbm, q_land.at[mz, mx], small_sem.at[2])
    own.start()

    @pl.when(root)
    def _():
        pl.semaphore_wait(barrier, nx - 1)

    @pl.when(me > 1)
    def _():
        pl.semaphore_wait(barrier, mz + mx - low.astype(jnp.int32))

    for z in range(top_z):
        @pl.when((z < mz) & direct(mz, z) & ((mx > 0) | (z > 0)))
        def _():
            pl.semaphore_signal(ready.at[mz], inc=1, device_id=at(z, mx), device_id_type=MESH)

    @pl.when((mx == 0) & ~low & direct(mz, 0))
    def _():
        pl.semaphore_signal(ready_low.at[mz], inc=1, device_id=at(0, 1), device_id_type=MESH)

    for x in range(nx - 1):
        @pl.when((x < mx) & ((x > 0) | ~low))
        def _():
            pl.semaphore_signal(x_ready.at[mx], inc=1, device_id=at(mz, x), device_id_type=MESH)

    small = [
        pltpu.make_async_copy(slot_hbm, slot, small_sem.at[0]),
        pltpu.make_async_copy(len_hbm, lens, small_sem.at[1]),
    ]
    loads = [pltpu.make_async_copy(k_hbm.at[s], kbuf.at[s], ksem.at[s]) for s in range(slots)]
    vloads = [pltpu.make_async_copy(v_hbm.at[s], vbuf.at[s], vsem.at[s]) for s in range(slots)]
    for c in small + loads + vloads:
        c.start()
    own.wait()
    first_row = q_land.at[0, 0]

    def row_copy(row, z, x, send, recv):
        return pltpu.make_async_remote_copy(
            src_ref=row, dst_ref=row, send_sem=send, recv_sem=recv, device_id=at(z, x), device_id_type=MESH)

    for x in range(nx):
        @pl.when((x > mx) & ~root)
        def _():
            pl.semaphore_wait(x_ready.at[x], 1)

        @pl.when((x != mx) & ((x > 0) | ~low) & ~root)
        def _():
            row_copy(q_land.at[mz, mx], mz, x, x_send_sem, x_recv_sem).start()

        @pl.when((x > 0) & root)
        def _():
            row_copy(first_row, 0, x, x_send_sem, root_sem).start()

    three = q_land.at[mz, pl.ds(0, nx - 1)]
    two = q_land.at[mz, pl.ds(0, nx - 2)]

    def piece(b):
        return q_land.at[0, pl.ds(1, nx - 1)] if isinstance(b, int) and b == 0 else q_land.at[b]

    def block_copy(b, z, x, sem):
        return row_copy(piece(b), z, x, sem, block_sem.at[b])

    def block_wait(b):
        pltpu.make_async_copy(piece(b), piece(b), block_sem.at[b]).wait()

    q_use[0, 0] = jnp.zeros((group, hd), BF16)

    @pl.when(low & ~root)
    def _():
        pltpu.make_async_copy(two, two, x_recv_sem).wait()

    @pl.when(~low)
    def _():
        pltpu.make_async_copy(three, three, x_recv_sem).wait()
        q_use[mz] = q_land[mz]

    for b in range(top_z):
        @pl.when((b < mz) & ((mx > 0) | (b > 0)))
        def _():
            block_copy(mz, b, mx, block_send.at[b]).start()

    for c in small:
        c.wait()
    per_seq = slots * n // nz
    code = [slot[s] for s in range(slots)]
    seq = [c // per_seq for c in code]
    col = lax.broadcasted_iota(jnp.int32, (1, slots * rows), 1)
    seq_at = jnp.zeros_like(col)
    for s in range(slots):
        seq_at = jnp.where(col // rows == s, seq[s], seq_at)
    r = lax.broadcasted_iota(jnp.int32, (nz * rows, slots * rows), 0)
    c = lax.broadcasted_iota(jnp.int32, (nz * rows, slots * rows), 1)
    wanted = r // (nz * group) * group + lax.rem(r, group)
    same = (lax.rem(r, nz * group) // group == seq_at) & (wanted == lax.rem(c, rows))
    gather[...] = jnp.where(same, 1.0, 0.0).astype(BF16)
    r = lax.broadcasted_iota(jnp.int32, (nz * half, slots * rows), 0)
    c = lax.broadcasted_iota(jnp.int32, (nz * half, slots * rows), 1)
    same = (lax.rem(r, nz) == seq_at) & (r // nz == lax.rem(c, rows) // group)
    gather_stat[...] = jnp.where(same, 1.0, 0.0).astype(BF16)

    for s in range(slots):
        loads[s].wait()
        for p in range(pairs):
            ktr[s, p] = kbuf[s, :, p].reshape(wide, hd).T
    for s in range(slots):
        vloads[s].wait()

    for z in range(1, nz):
        @pl.when((z > mz) & direct(z, mz) & ~root)
        def _():
            pl.semaphore_wait(ready.at[z], 1)

            @pl.when(~low)
            def _():
                block_copy(mz, z, mx, block_send.at[z]).start()

            @pl.when(low)
            def _():
                block_copy(0, z, mx, block_send.at[z]).start()

        if direct(z, 0):
            @pl.when(agent)
            def _():
                pl.semaphore_wait(ready_low.at[z], 1)
                block_copy(0, z, 0, col_send.at[z]).start()

        if z > reach:
            @pl.when(z == mz + reach)
            def _():
                for b in range(max(0, z - reach - nz // 2 + 1), z - reach):
                    block_wait(b)
                    block_copy(b, z, mx, relay_send.at[b]).start()

    @pl.when(low & ~root)
    def _():
        pltpu.make_async_copy(first_row, first_row, root_sem).wait()

    for z in range(1, nz):
        @pl.when(low & ~root)
        def _():
            row_copy(first_row, z, mx, row_send.at[z], root_sem).start()

        @pl.when(agent)
        def _():
            row_copy(first_row, z, 0, row_send_low.at[z], root_sem).start()

    @pl.when(agent)
    def _():
        block_copy(0, 0, 0, root_send.at[0]).start()

    def first(b):
        return ((b <= mz) & (mz >= reach)).astype(jnp.int32)

    def goes(b, late):
        return jnp.where((mx == 0) & (b == 0), late == 1, first(b) != late)

    scale = hd ** -0.5 * math.log2(math.e)

    def to_rows(f):
        r = lax.broadcasted_iota(jnp.int32, (nz * group, hd), 0)
        c = lax.broadcasted_iota(jnp.int32, (nz * group, hd), 1)
        spread = jnp.broadcast_to(f[:, None, :], (nz, group, hd)).reshape(nz * group, hd)
        return jnp.sum(jnp.where(lax.rem(r, group) == c, spread, 0.0), axis=1, keepdims=True)

    def one_pass(late, carry):
        for b in range(nz):
            @pl.when((first(b) != late) & ((b != mz) | root) & ~relayed(b))
            def _():
                block_wait(b)

            if b > 0:
                @pl.when(agent)
                def _():
                    block_copy(b, 0, 0, root_send.at[b]).start()

                @pl.when((first(b) != late) & (b != mz))
                def _():
                    q_use[b] = q_land[b]
            else:
                @pl.when(first(b) != late)
                def _():
                    q_use[0, pl.ds(1, nx - 1)] = q_land[0, pl.ds(1, nx - 1)]

        @pl.when(late == 1)
        def _():
            @pl.when(~low)
            def _():
                pltpu.make_async_copy(first_row, first_row, root_sem).wait()

            q_use[0, 0] = q_land[0, 0]

        lane = lax.broadcasted_iota(jnp.int32, (rows, wide), 1)
        row = lax.broadcasted_iota(jnp.int32, (rows, wide), 0)
        matched = lax.rem(lane, half) == row // group
        token = jnp.where(matched, lane // half, block)
        left = []
        for b, c in zip(seq, code):
            rest = jnp.clip(lens[b] - lax.rem(c, per_seq) * block, 0, block)
            ours = (first(b) != late) | ((b == 0) & (late == 1))
            left.append(jnp.where(ours, rest, 0))
        for p in range(pairs):
            peak, total, part = [], [], []
            for s in range(slots):
                q = q_use[seq[s], pl.ds(p * half, half)].reshape(rows, hd)
                sc = jnp.dot(q, ktr[s, p], preferred_element_type=F32)
                live = token < left[s]
                sc = jnp.where(live, sc, NEG)
                m = jnp.max(sc, axis=1, keepdims=True)
                w = jnp.where(live, jnp.exp2((sc - m) * scale), 0.0).astype(BF16)
                total.append(jnp.broadcast_to(jnp.sum(w.astype(F32), axis=1, keepdims=True), (rows, hd)))
                part.append(jnp.dot(w, vbuf[s, :, p].reshape(wide, hd), preferred_element_type=F32))
                peak.append(jnp.broadcast_to(m, (rows, hd)))
            stats = []
            for s in range(slots):
                best = peak[s]
                for t in range(slots):
                    if t != s:
                        best = jnp.maximum(best, jnp.where(seq[t] == seq[s], peak[t], NEG))
                f = jnp.exp2((peak[s] - best) * scale)
                part[s] = part[s] * f
                total[s] = total[s] * f
                head = lax.broadcasted_iota(jnp.int32, (rows, hd), 1) - lax.rem(
                    lax.broadcasted_iota(jnp.int32, (rows, hd), 0), group)
                lead = best
                for t in range(s):
                    lead = jnp.where(seq[t] == seq[s], 0.0, lead)
                stats.append(jnp.where(head == 0, lead, 0.0) + jnp.where(head == group, total[s], 0.0))
            both = jnp.concatenate(part, axis=0).astype(BF16)
            acc = jnp.dot(gather[...], both, preferred_element_type=F32).astype(BF16)
            for e in range(half):
                out_send[late, p * half + e] = acc[e * nz * group:(e + 1) * nz * group]
            rest = jnp.concatenate(stats, axis=0)
            st = jnp.zeros((nz * half, hd), F32)
            for _ in range(3):
                piece = rest.astype(BF16)
                st = st + jnp.dot(gather_stat[...], piece, preferred_element_type=F32)
                rest = rest - piece.astype(F32)
            for e in range(half):
                st_send[late, p * half + e] = st[e * nz:(e + 1) * nz]
        for x in range(nx):
            @pl.when(x != mx)
            def _():
                pltpu.make_async_remote_copy(
                    src_ref=out_send.at[late, x], dst_ref=out_recv.at[late, mx],
                    send_sem=o_send_sem.at[late], recv_sem=o_recv_sem.at[late],
                    device_id=at(mz, x), device_id_type=MESH).start()
                pltpu.make_async_remote_copy(
                    src_ref=st_send.at[late, x], dst_ref=st_recv.at[late, mx],
                    send_sem=s_send_sem.at[late], recv_sem=s_recv_sem.at[late],
                    device_id=at(mz, x), device_id_type=MESH).start()
        out_recv[late, mx] = out_send[late, mx]
        st_recv[late, mx] = st_send[late, mx]
        peers_o = out_recv.at[late, pl.ds(0, nx - 1)]
        peers_s = st_recv.at[late, pl.ds(0, nx - 1)]
        pltpu.make_async_copy(peers_s, peers_s, s_recv_sem.at[late]).wait()
        pltpu.make_async_copy(peers_o, peers_o, o_recv_sem.at[late]).wait()

        stat = [st_recv[late, x] for x in range(nx)]
        total = [pltpu.roll(v, hd - group, 1) for v in stat]
        stat = [jnp.where(t > 0.0, v, NEG) for v, t in zip(stat, total)]
        best = functools.reduce(jnp.maximum, stat)
        f = [jnp.exp2((v - best) * scale) for v in stat]
        den = sum(g * t for g, t in zip(f, total))
        acc = sum(to_rows(f[x]) * out_recv[late, x].astype(F32) for x in range(nx))
        z_send[late] = acc.reshape(nz, group, hd)
        lane = lax.broadcasted_iota(jnp.int32, (nz, hd), 1)
        both = jnp.where(lane < group, best, jnp.where(lane < 2 * group, pltpu.roll(den, group, 1), 0.0))
        zs_send[late] = both.reshape(nz, 1, hd)
        for b in range(nz):
            @pl.when(goes(b, late) & (b != mz))
            def _():
                pltpu.make_async_remote_copy(
                    src_ref=z_send.at[late, b], dst_ref=z_recv.at[mz], send_sem=z_send_sem, recv_sem=z_recv_sem,
                    device_id=at(b, mx), device_id_type=MESH).start()
                pltpu.make_async_remote_copy(
                    src_ref=zs_send.at[late, b], dst_ref=zs_recv.at[mz], send_sem=zs_send_sem, recv_sem=zs_recv_sem,
                    device_id=at(b, mx), device_id_type=MESH).start()

        pltpu.make_async_copy(peers_s, peers_s, s_send_sem.at[late]).wait()
        pltpu.make_async_copy(peers_o, peers_o, o_send_sem.at[late]).wait()
        return carry

    lax.fori_loop((mz < reach).astype(jnp.int32), 2, one_pass, 0)
    last = (mz < reach).astype(jnp.int32)
    z_recv[mz] = z_send[last, mz]
    zs_recv[mz] = zs_send[last, mz]
    rest_s = zs_recv.at[pl.ds(0, nz - 1)]
    rest_z = z_recv.at[pl.ds(0, nz - 1)]
    pltpu.make_async_copy(rest_s, rest_s, zs_recv_sem).wait()
    pltpu.make_async_copy(rest_z, rest_z, z_recv_sem).wait()

    stat = zs_recv[...].reshape(nz, hd)
    total = pltpu.roll(stat, hd - group, 1)
    stat = jnp.where(total > 0.0, stat, NEG)
    best = jnp.max(stat, axis=0, keepdims=True)
    f = jnp.exp2((stat - best) * scale)
    f = f / jnp.sum(f * total, axis=0, keepdims=True)
    acc = to_rows(f) * z_recv[...].reshape(nz * group, hd)
    o_ref[...] = jnp.sum(acc.reshape(nz, group, hd), axis=0).astype(BF16)

    @pl.when(low & ~root)
    def _():
        pltpu.make_async_copy(two, two, x_send_sem).wait()

    @pl.when(root | ~low)
    def _():
        pltpu.make_async_copy(three, three, x_send_sem).wait()

    for z in range(nz):
        @pl.when(~low & (z != mz) & (((z < mz) & ((mx > 0) | (z > 0))) | ((z > mz) & direct(z, mz))))
        def _():
            block_copy(mz, z, mx, block_send.at[z]).wait_send()

        @pl.when(relayed(z))
        def _():
            block_copy(z, 0, mx, relay_send.at[z]).wait_send()

        @pl.when(agent)
        def _():
            block_copy(z, 0, 0, root_send.at[z]).wait_send()

        if z > 0:
            @pl.when(low & ~root)
            def _():
                row_copy(first_row, z, mx, row_send.at[z], root_sem).wait_send()

            @pl.when(agent)
            def _():
                row_copy(first_row, z, 0, row_send_low.at[z], root_sem).wait_send()

            if direct(z, 0):
                @pl.when(low & ~root)
                def _():
                    block_copy(0, z, mx, block_send.at[z]).wait_send()

                @pl.when(agent)
                def _():
                    block_copy(0, z, 0, col_send.at[z]).wait_send()

    pltpu.make_async_copy(rest_z, rest_z, z_send_sem).wait()
    pltpu.make_async_copy(rest_s, rest_s, zs_send_sem).wait()


def solution(mesh):
    n = mesh.shape["seq"]

    def body(queries, keys, values, lengths, slot_block):
        share, _, hd = queries.shape
        slots, block, kv_local, _ = keys.shape
        nz = lengths.shape[0]
        nx = n // nz
        half = 2
        group = share
        split = (slots, block, nx // half, half, hd)
        any_ = pl.BlockSpec(memory_space=pl.ANY)
        dims = (nz, nx, slots, block, group, hd)
        dma, regular = pltpu.SemaphoreType.DMA, pltpu.SemaphoreType.REGULAR
        out = pl.pallas_call(
            functools.partial(attend, dims),
            out_shape=jax.ShapeDtypeStruct((share, hd), BF16),
            in_specs=[any_] * 5,
            out_specs=pl.BlockSpec(memory_space=pltpu.VMEM),
            scratch_shapes=[
                pltpu.VMEM(split, BF16), pltpu.VMEM(split, BF16),
                pltpu.VMEM((slots, nx // half, hd, block * half), BF16),
                pltpu.VMEM((nz * half * share, slots * half * share), BF16),
                pltpu.VMEM((nz * half, slots * half * share), BF16),
                pltpu.VMEM((nz, nx, share, hd), BF16), pltpu.VMEM((nz, nx, share, hd), BF16),
                pltpu.SMEM((nz,), jnp.int32), pltpu.SMEM((slots,), jnp.int32),
                pltpu.VMEM((2, nx, nz * share, hd), BF16), pltpu.VMEM((2, nx, nz * share, hd), BF16),
                pltpu.VMEM((2, nx, nz, hd), F32), pltpu.VMEM((2, nx, nz, hd), F32),
                pltpu.VMEM((2, nz, share, hd), F32), pltpu.VMEM((nz, share, hd), F32),
                pltpu.VMEM((2, nz, 1, hd), F32), pltpu.VMEM((nz, 1, hd), F32),
                dma((slots,)), dma((slots,)), dma((3,)), regular((nz,)), regular((nz,)), regular((nx,)), dma, dma((nz,)), dma((nz,)), dma((nz,)), dma((nz,)), dma, dma,
                dma((nz,)), dma((nz,)), dma((nz,)), dma((2,)), dma((2,)), dma((2,)), dma((2,)), dma, dma, dma, dma,
            ],
            compiler_params=pltpu.CompilerParams(collective_id=0, has_side_effects=True),
        )(queries.reshape(share, hd), keys.reshape(split), values.reshape(split), lengths, slot_block)
        return out.reshape(share, 1, hd)

    placed = (
        P(("grp", "seq"), "head", None),
        P(("grp", "seq"), None, "head", None),
        P(("grp", "seq"), None, "head", None),
        P("grp"),
        P(("grp", "seq")),
    )
    return jax.shard_map(
        body, mesh=mesh, in_specs=placed, out_specs=P(("grp", "seq"), "head", None), check_vma=False
    )
```

```python
import functools
import math

import jax
import jax.numpy as jnp
from jax import lax
from jax.experimental import pallas as pl
from jax.experimental.pallas import tpu as pltpu
from jax.sharding import PartitionSpec as P

MESH = pl.DeviceIdType.MESH
F32 = jnp.float32
BF16 = jnp.bfloat16
NEG = -1e30


def attend(dims, q_hbm, k_hbm, v_hbm, len_hbm, slot_hbm, o_ref,
           kbuf, vbuf, ktr, gather, gather_stat, q_land, q_use, lens, slot, out_send, out_recv, st_send, st_recv,
           ksem, vsem, small_sem, ready, ready_low, x_ready, root_sem, row_send, row_send_low, root_send, col_send, x_send_sem, x_recv_sem, block_send, block_sem,
           o_send_sem, o_recv_sem, s_send_sem, s_recv_sem):
    nz, nx, slots, block, group, hd = dims
    n = nz * nx
    half = 2
    pairs = nx // half
    rows = half * group
    wide = block * half
    me = lax.axis_index("seq")
    mz, mx = me // nx, lax.rem(me, nx)
    top_z = nz - 1

    reach = nz // 4
    middle = nz // 2

    def at(z, x):
        return {"seq": z * nx + x}

    low = mz == 0
    root = me == 0
    agent = me == 1

    barrier = pltpu.get_barrier_semaphore()

    def greet(z, x):
        pl.semaphore_signal(barrier, inc=1, device_id=at(z, x), device_id_type=MESH)

    for z in range(top_z, 0, -1):
        @pl.when((z > mz) & ~root)
        def _():
            greet(z, mx)

        @pl.when(agent)
        def _():
            greet(z, 0)

    for x in range(nx):
        @pl.when(((x > mx) & ~root) | ((x == 0) & low & ~root))
        def _():
            greet(mz, x)

    own = pltpu.make_async_copy(q_hbm, q_land.at[mz, mx], small_sem.at[2])
    own.start()

    @pl.when(root)
    def _():
        pl.semaphore_wait(barrier, nx - 1)

    @pl.when(me > 1)
    def _():
        pl.semaphore_wait(barrier, mz + mx - low.astype(jnp.int32))

    for z in range(top_z):
        @pl.when((z < mz) & ((mx > 0) | (z > 0)))
        def _():
            pl.semaphore_signal(ready.at[mz], inc=1, device_id=at(z, mx), device_id_type=MESH)

    @pl.when((mx == 0) & ~low)
    def _():
        pl.semaphore_signal(ready_low.at[mz], inc=1, device_id=at(0, 1), device_id_type=MESH)

    for x in range(nx - 1):
        @pl.when((x < mx) & ((x > 0) | ~low))
        def _():
            pl.semaphore_signal(x_ready.at[mx], inc=1, device_id=at(mz, x), device_id_type=MESH)

    small = [
        pltpu.make_async_copy(slot_hbm, slot, small_sem.at[0]),
        pltpu.make_async_copy(len_hbm, lens, small_sem.at[1]),
    ]
    loads = [pltpu.make_async_copy(k_hbm.at[s], kbuf.at[s], ksem.at[s]) for s in range(slots)]
    vloads = [pltpu.make_async_copy(v_hbm.at[s], vbuf.at[s], vsem.at[s]) for s in range(slots)]
    for c in small + loads + vloads:
        c.start()
    own.wait()
    first_row = q_land.at[0, 0]

    def row_copy(row, z, x, send, recv):
        return pltpu.make_async_remote_copy(
            src_ref=row, dst_ref=row, send_sem=send, recv_sem=recv, device_id=at(z, x), device_id_type=MESH)

    for x in range(nx):
        @pl.when((x > mx) & ~root)
        def _():
            pl.semaphore_wait(x_ready.at[x], 1)

        @pl.when((x != mx) & ((x > 0) | ~low) & ~root)
        def _():
            row_copy(q_land.at[mz, mx], mz, x, x_send_sem, x_recv_sem).start()

        @pl.when((x > 0) & root)
        def _():
            row_copy(first_row, 0, x, x_send_sem, root_sem).start()

    three = q_land.at[mz, pl.ds(0, nx - 1)]
    two = q_land.at[mz, pl.ds(0, nx - 2)]

    def piece(b):
        return q_land.at[0, pl.ds(1, nx - 1)] if isinstance(b, int) and b == 0 else q_land.at[b]

    def block_copy(b, z, x, sem):
        return row_copy(piece(b), z, x, sem, block_sem.at[b])

    def block_wait(b):
        pltpu.make_async_copy(piece(b), piece(b), block_sem.at[b]).wait()

    q_use[0, 0] = jnp.zeros((group, hd), BF16)

    @pl.when(low & ~root)
    def _():
        pltpu.make_async_copy(two, two, x_recv_sem).wait()

    @pl.when(~low)
    def _():
        pltpu.make_async_copy(three, three, x_recv_sem).wait()
        q_use[mz] = q_land[mz]

    for b in range(top_z):
        @pl.when((b < mz) & ((mx > 0) | (b > 0)))
        def _():
            block_copy(mz, b, mx, block_send.at[b]).start()

    for z in range(1, nz):
        @pl.when((z > mz) & ~root)
        def _():
            pl.semaphore_wait(ready.at[z], 1)

            @pl.when(~low)
            def _():
                block_copy(mz, z, mx, block_send.at[z]).start()

            @pl.when(low)
            def _():
                block_copy(0, z, mx, block_send.at[z]).start()

        @pl.when(agent)
        def _():
            pl.semaphore_wait(ready_low.at[z], 1)
            block_copy(0, z, 0, col_send.at[z]).start()

    @pl.when(low & ~root)
    def _():
        pltpu.make_async_copy(first_row, first_row, root_sem).wait()

    for z in range(1, nz):
        @pl.when(low & ~root)
        def _():
            row_copy(first_row, z, mx, row_send.at[z], root_sem).start()

        @pl.when(agent)
        def _():
            row_copy(first_row, z, 0, row_send_low.at[z], root_sem).start()

    @pl.when(agent)
    def _():
        block_copy(0, 0, 0, root_send.at[0]).start()

    for c in small:
        c.wait()
    per_seq = slots * n // nz
    code = [slot[s] for s in range(slots)]
    seq = [c // per_seq for c in code]
    col = lax.broadcasted_iota(jnp.int32, (1, slots * rows), 1)
    seq_at = jnp.zeros_like(col)
    for s in range(slots):
        seq_at = jnp.where(col // rows == s, seq[s], seq_at)
    r = lax.broadcasted_iota(jnp.int32, (nz * rows, slots * rows), 0)
    c = lax.broadcasted_iota(jnp.int32, (nz * rows, slots * rows), 1)
    wanted = r // (nz * group) * group + lax.rem(r, group)
    same = (lax.rem(r, nz * group) // group == seq_at) & (wanted == lax.rem(c, rows))
    gather[...] = jnp.where(same, 1.0, 0.0).astype(BF16)
    lane_slot = lax.broadcasted_iota(jnp.int32, (1, hd), 1)
    lane_seq = jnp.full((1, hd), -1, jnp.int32)
    lane_lead = jnp.zeros((1, hd), jnp.int32)
    for s in range(slots):
        lead = 1
        for t in range(s):
            lead = lead * (seq[t] != seq[s]).astype(jnp.int32)
        lane_seq = jnp.where(lax.rem(lane_slot, slots) == s, seq[s], lane_seq)
        lane_lead = jnp.where(lane_slot == s, lead, lane_lead)
    lane_seq = jnp.where(lane_slot < 3 * slots, lane_seq, -1)
    r = lax.broadcasted_iota(jnp.int32, (nz, hd), 0)
    gather_stat[...] = jnp.where(r == lane_seq, 1.0, 0.0).astype(BF16)

    for s in range(slots):
        loads[s].wait()
        for p in range(pairs):
            ktr[s, p] = kbuf[s, :, p].reshape(wide, hd).T
    for s in range(slots):
        vloads[s].wait()

    row_pass = (mz < middle).astype(jnp.int32)

    def first(b):
        d = jnp.abs(mz - b)
        near = jnp.minimum(d, nz - d) <= jnp.maximum(nz - mz, reach + 1)
        return ((b <= mz) & (mz >= reach) & near).astype(jnp.int32)

    def goes(b, x, late):
        return late == row_pass if b == 0 and x == 0 else first(b) != late

    scale = hd ** -0.5 * math.log2(math.e)

    def one_pass(late, carry):
        for b in range(nz):
            @pl.when((first(b) != late) & ((b != mz) | root))
            def _():
                block_wait(b)

            if b > 0:
                @pl.when(agent)
                def _():
                    block_copy(b, 0, 0, root_send.at[b]).start()

                @pl.when((first(b) != late) & (b != mz))
                def _():
                    q_use[b] = q_land[b]
            else:
                @pl.when(first(b) != late)
                def _():
                    q_use[0, pl.ds(1, nx - 1)] = q_land[0, pl.ds(1, nx - 1)]

        @pl.when(late == row_pass)
        def _():
            @pl.when(~low)
            def _():
                pltpu.make_async_copy(first_row, first_row, root_sem).wait()

            q_use[0, 0] = q_land[0, 0]

        lane = lax.broadcasted_iota(jnp.int32, (rows, wide), 1)
        row = lax.broadcasted_iota(jnp.int32, (rows, wide), 0)
        matched = lax.rem(lane, half) == row // group
        token = jnp.where(matched, lane // half, block)
        left = []
        for b, c in zip(seq, code):
            rest = jnp.clip(lens[b] - lax.rem(c, per_seq) * block, 0, block)
            ours = (first(b) != late) | ((b == 0) & (late == row_pass))
            left.append(jnp.where(ours, rest, 0))
        for p in range(pairs):
            peak, total, part = [], [], []
            for s in range(slots):
                q = q_use[seq[s], pl.ds(p * half, half)].reshape(rows, hd)
                sc = jnp.dot(q, ktr[s, p], preferred_element_type=F32)
                live = token < left[s]
                sc = jnp.where(live, sc, NEG)
                m = jnp.max(sc, axis=1, keepdims=True)
                w = jnp.where(live, jnp.exp2((sc - m) * scale), 0.0).astype(BF16)
                total.append(jnp.sum(w.astype(F32), axis=1, keepdims=True))
                part.append(jnp.dot(w, vbuf[s, :, p].reshape(wide, hd), preferred_element_type=F32))
                peak.append(m)
            lane_s = lax.broadcasted_iota(jnp.int32, (rows, hd), 1)
            tops = jnp.full((rows, hd), NEG, F32)
            sums = jnp.zeros((rows, hd), F32)
            best = jnp.full((rows, hd), NEG, F32)
            for s in range(slots):
                tops = jnp.where(lane_s == s, peak[s], tops)
                sums = jnp.where(lane_s == s, total[s], sums)
                best = jnp.maximum(best, jnp.where(lane_seq == seq[s], peak[s], NEG))
            f = jnp.exp2((tops - best) * scale)
            sums = sums * f
            lead = jnp.where(lane_lead == 1, best, 0.0)
            both = jnp.concatenate([part[s] * f[:, s:s + 1] for s in range(slots)], axis=0).astype(BF16)
            acc = jnp.dot(gather[...], both, preferred_element_type=F32)
            for e in range(half):
                half_acc = acc[e * nz * group:(e + 1) * nz * group].reshape(nz, group, hd)
                out_send[late, p * half + e] = half_acc.astype(BF16)
            mixed = []
            for e in range(half):
                mixed += [lead[e * group:(e + 1) * group], sums[e * group:(e + 1) * group]]
            rest = jnp.concatenate(mixed + [jnp.zeros((hd - 2 * rows, hd), F32)], axis=0)
            packed = jnp.zeros((hd, hd), F32)
            for k in range(3):
                coarse = rest.astype(BF16).astype(F32)
                packed = packed + (pltpu.roll(coarse, k * slots, 1) if k else coarse)
                rest = rest - coarse
            st = lax.dot_general(
                gather_stat[...], packed.astype(BF16), (((1,), (1,)), ((), ())), preferred_element_type=F32)
            st_send[late, p] = st.reshape(nz, 1, hd)
        for b in range(nz):
            for x in range(nx):
                @pl.when(goes(b, x, late) & (b * nx + x != me))
                def _():
                    pltpu.make_async_remote_copy(
                        src_ref=out_send.at[late, x, b], dst_ref=out_recv.at[me],
                        send_sem=o_send_sem, recv_sem=o_recv_sem,
                        device_id=at(b, x), device_id_type=MESH).start()
                    pltpu.make_async_remote_copy(
                        src_ref=st_send.at[late, x // half, b], dst_ref=st_recv.at[me],
                        send_sem=s_send_sem, recv_sem=s_recv_sem,
                        device_id=at(b, x), device_id_type=MESH).start()
        return carry

    lax.fori_loop((mz < reach).astype(jnp.int32), 2, one_pass, 0)
    last = (mz < reach).astype(jnp.int32)
    out_recv[me] = out_send[last, mx, mz]
    st_recv[me] = st_send[last, mx // half, mz]
    rest_s = st_recv.at[pl.ds(0, n - 1)]
    rest_o = out_recv.at[pl.ds(0, n - 1)]
    pltpu.make_async_copy(rest_s, rest_s, s_recv_sem).wait()
    pltpu.make_async_copy(rest_o, rest_o, o_recv_sem).wait()

    stat = st_recv[...].reshape(n, hd)
    stat = jnp.where(lax.rem(mx, half) == 1, pltpu.roll(stat, hd - 2 * group, 1), stat)
    total = pltpu.roll(stat, hd - group, 1)
    stat = jnp.where(total > 0.0, stat, NEG)
    best = jnp.max(stat, axis=0, keepdims=True)
    f = jnp.exp2((stat - best) * scale)
    f = f / jnp.sum(f * total, axis=0, keepdims=True)
    r = lax.broadcasted_iota(jnp.int32, (group, hd), 0)
    c = lax.broadcasted_iota(jnp.int32, (group, hd), 1)
    acc = jnp.zeros((group, hd), F32)
    for i in range(n):
        g = jnp.where(c == r, jnp.broadcast_to(f[i:i + 1], (group, hd)), 0.0)
        acc = acc + jnp.sum(g, axis=1, keepdims=True) * out_recv[i].astype(F32)
    o_ref[...] = acc.astype(BF16)

    @pl.when(low & ~root)
    def _():
        pltpu.make_async_copy(two, two, x_send_sem).wait()

    @pl.when(root | ~low)
    def _():
        pltpu.make_async_copy(three, three, x_send_sem).wait()

    for z in range(nz):
        @pl.when(~low & (z != mz) & (((z < mz) & ((mx > 0) | (z > 0))) | (z > mz)))
        def _():
            block_copy(mz, z, mx, block_send.at[z]).wait_send()

        @pl.when(agent)
        def _():
            block_copy(z, 0, 0, root_send.at[z]).wait_send()

        if z > 0:
            @pl.when(low & ~root)
            def _():
                row_copy(first_row, z, mx, row_send.at[z], root_sem).wait_send()

            @pl.when(agent)
            def _():
                row_copy(first_row, z, 0, row_send_low.at[z], root_sem).wait_send()

            @pl.when(low & ~root)
            def _():
                block_copy(0, z, mx, block_send.at[z]).wait_send()

            @pl.when(agent)
            def _():
                block_copy(0, z, 0, col_send.at[z]).wait_send()

    pltpu.make_async_copy(rest_o, rest_o, o_send_sem).wait()
    pltpu.make_async_copy(rest_s, rest_s, s_send_sem).wait()


def solution(mesh):
    n = mesh.shape["seq"]

    def body(queries, keys, values, lengths, slot_block):
        share, _, hd = queries.shape
        slots, block, kv_local, _ = keys.shape
        nz = lengths.shape[0]
        nx = n // nz
        half = 2
        group = share
        split = (slots, block, nx // half, half, hd)
        any_ = pl.BlockSpec(memory_space=pl.ANY)
        dims = (nz, nx, slots, block, group, hd)
        dma, regular = pltpu.SemaphoreType.DMA, pltpu.SemaphoreType.REGULAR
        out = pl.pallas_call(
            functools.partial(attend, dims),
            out_shape=jax.ShapeDtypeStruct((share, hd), BF16),
            in_specs=[any_] * 5,
            out_specs=pl.BlockSpec(memory_space=pltpu.VMEM),
            scratch_shapes=[
                pltpu.VMEM(split, BF16), pltpu.VMEM(split, BF16),
                pltpu.VMEM((slots, nx // half, hd, block * half), BF16),
                pltpu.VMEM((nz * half * share, slots * half * share), BF16),
                pltpu.VMEM((nz, hd), BF16),
                pltpu.VMEM((nz, nx, share, hd), BF16), pltpu.VMEM((nz, nx, share, hd), BF16),
                pltpu.SMEM((nz,), jnp.int32), pltpu.SMEM((slots,), jnp.int32),
                pltpu.VMEM((2, nx, nz, share, hd), BF16), pltpu.VMEM((n, share, hd), BF16),
                pltpu.VMEM((2, nx // half, nz, 1, hd), F32), pltpu.VMEM((n, 1, hd), F32),
                dma((slots,)), dma((slots,)), dma((3,)), regular((nz,)), regular((nz,)), regular((nx,)), dma, dma((nz,)), dma((nz,)), dma((nz,)), dma((nz,)), dma, dma,
                dma((nz,)), dma((nz,)), dma, dma, dma, dma,
            ],
            compiler_params=pltpu.CompilerParams(collective_id=0, has_side_effects=True),
        )(queries.reshape(share, hd), keys.reshape(split), values.reshape(split), lengths, slot_block)
        return out.reshape(share, 1, hd)

    placed = (
        P(("grp", "seq"), "head", None),
        P(("grp", "seq"), None, "head", None),
        P(("grp", "seq"), None, "head", None),
        P("grp"),
        P(("grp", "seq")),
    )
    return jax.shard_map(
        body, mesh=mesh, in_specs=placed, out_specs=P(("grp", "seq"), "head", None), check_vma=False
    )
```

```python
import functools
import math

import jax
import jax.numpy as jnp
from jax import lax
from jax.experimental import pallas as pl
from jax.experimental.pallas import tpu as pltpu
from jax.sharding import PartitionSpec as P

MESH = pl.DeviceIdType.MESH
F32 = jnp.float32
BF16 = jnp.bfloat16
NEG = -1e30


def attend(dims, q_hbm, k_hbm, v_hbm, len_hbm, slot_hbm, o_ref,
           kbuf, vbuf, ktr, gather, gather_stat, q_land, q_use, lens, slot, out_send, out_recv, st_send, st_recv,
           ksem, vsem, small_sem, ready, ready_low, x_ready, root_sem, row_send, row_send_low, root_send, col_send, x_send_sem, x_recv_sem, block_send, block_sem,
           o_send_sem, o_recv_sem, s_send_sem, s_recv_sem):
    nz, nx, slots, block, group, hd = dims
    n = nz * nx
    half = 2
    pairs = nx // half
    rows = half * group
    wide = block * half
    me = lax.axis_index("seq")
    mz, mx = me // nx, lax.rem(me, nx)
    top_z = nz - 1

    reach = nz // 4
    middle = nz // 2

    def at(z, x):
        return {"seq": z * nx + x}

    low = mz == 0
    root = me == 0
    agent = me == 1

    barrier = pltpu.get_barrier_semaphore()

    def greet(z, x):
        pl.semaphore_signal(barrier, inc=1, device_id=at(z, x), device_id_type=MESH)

    for z in range(top_z, 0, -1):
        @pl.when((z > mz) & ~root)
        def _():
            greet(z, mx)

        @pl.when(agent)
        def _():
            greet(z, 0)

    for x in range(nx):
        @pl.when(((x > mx) & ~root) | ((x == 0) & low & ~root))
        def _():
            greet(mz, x)

    own = pltpu.make_async_copy(q_hbm, q_land.at[mz, mx], small_sem.at[2])
    own.start()

    @pl.when(root)
    def _():
        pl.semaphore_wait(barrier, nx - 1)

    @pl.when(me > 1)
    def _():
        pl.semaphore_wait(barrier, mz + mx - low.astype(jnp.int32))

    for z in range(top_z):
        @pl.when((z < mz) & ((mx > 0) | (z > 0)))
        def _():
            pl.semaphore_signal(ready.at[mz], inc=1, device_id=at(z, mx), device_id_type=MESH)

    @pl.when((mx == 0) & ~low)
    def _():
        pl.semaphore_signal(ready_low.at[mz], inc=1, device_id=at(0, 1), device_id_type=MESH)

    for x in range(nx - 1):
        @pl.when((x < mx) & ((x > 0) | ~low))
        def _():
            pl.semaphore_signal(x_ready.at[mx], inc=1, device_id=at(mz, x), device_id_type=MESH)

    small = [
        pltpu.make_async_copy(slot_hbm, slot, small_sem.at[0]),
        pltpu.make_async_copy(len_hbm, lens, small_sem.at[1]),
    ]
    loads = [pltpu.make_async_copy(k_hbm.at[s], kbuf.at[s], ksem.at[s]) for s in range(slots)]
    vloads = [pltpu.make_async_copy(v_hbm.at[s], vbuf.at[s], vsem.at[s]) for s in range(slots)]
    for c in small + loads + vloads:
        c.start()
    own.wait()
    first_row = q_land.at[0, 0]

    def row_copy(row, z, x, send, recv):
        return pltpu.make_async_remote_copy(
            src_ref=row, dst_ref=row, send_sem=send, recv_sem=recv, device_id=at(z, x), device_id_type=MESH)

    for x in range(nx):
        @pl.when((x > mx) & ~root)
        def _():
            pl.semaphore_wait(x_ready.at[x], 1)

        @pl.when((x != mx) & ((x > 0) | ~low) & ~root)
        def _():
            row_copy(q_land.at[mz, mx], mz, x, x_send_sem, x_recv_sem).start()

        @pl.when((x > 0) & root)
        def _():
            row_copy(first_row, 0, x, x_send_sem, root_sem).start()

    three = q_land.at[mz, pl.ds(0, nx - 1)]
    two = q_land.at[mz, pl.ds(0, nx - 2)]

    def piece(b):
        return q_land.at[0, pl.ds(1, nx - 1)] if isinstance(b, int) and b == 0 else q_land.at[b]

    def block_copy(b, z, x, sem):
        return row_copy(piece(b), z, x, sem, block_sem.at[b])

    def block_wait(b):
        pltpu.make_async_copy(piece(b), piece(b), block_sem.at[b]).wait()

    q_use[0, 0] = jnp.zeros((group, hd), BF16)

    @pl.when(low & ~root)
    def _():
        pltpu.make_async_copy(two, two, x_recv_sem).wait()

    @pl.when(~low)
    def _():
        pltpu.make_async_copy(three, three, x_recv_sem).wait()
        q_use[mz] = q_land[mz]

    for b in range(top_z):
        @pl.when((b < mz) & ((mx > 0) | (b > 0)))
        def _():
            block_copy(mz, b, mx, block_send.at[b]).start()

    for z in range(1, nz):
        @pl.when((z > mz) & ~root)
        def _():
            pl.semaphore_wait(ready.at[z], 1)

            @pl.when(~low)
            def _():
                block_copy(mz, z, mx, block_send.at[z]).start()

            @pl.when(low)
            def _():
                block_copy(0, z, mx, block_send.at[z]).start()

        @pl.when(agent)
        def _():
            pl.semaphore_wait(ready_low.at[z], 1)
            block_copy(0, z, 0, col_send.at[z]).start()

    @pl.when(low & ~root)
    def _():
        pltpu.make_async_copy(first_row, first_row, root_sem).wait()

    for z in range(1, nz):
        @pl.when(low & ~root)
        def _():
            row_copy(first_row, z, mx, row_send.at[z], root_sem).start()

        @pl.when(agent)
        def _():
            row_copy(first_row, z, 0, row_send_low.at[z], root_sem).start()

    @pl.when(agent)
    def _():
        block_copy(0, 0, 0, root_send.at[0]).start()

    for c in small:
        c.wait()
    per_seq = slots * n // nz
    code = [slot[s] for s in range(slots)]
    seq = [c // per_seq for c in code]
    col = lax.broadcasted_iota(jnp.int32, (1, slots * rows), 1)
    seq_at = jnp.zeros_like(col)
    for s in range(slots):
        seq_at = jnp.where(col // rows == s, seq[s], seq_at)
    r = lax.broadcasted_iota(jnp.int32, (nz * rows, slots * rows), 0)
    c = lax.broadcasted_iota(jnp.int32, (nz * rows, slots * rows), 1)
    wanted = r // (nz * group) * group + lax.rem(r, group)
    same = (lax.rem(r, nz * group) // group == seq_at) & (wanted == lax.rem(c, rows))
    gather[...] = jnp.where(same, 1.0, 0.0).astype(BF16)
    lane_slot = lax.broadcasted_iota(jnp.int32, (1, hd), 1)
    lane_seq = jnp.full((1, hd), -1, jnp.int32)
    lane_lead = jnp.zeros((1, hd), jnp.int32)
    for s in range(slots):
        lead = 1
        for t in range(s):
            lead = lead * (seq[t] != seq[s]).astype(jnp.int32)
        lane_seq = jnp.where(lax.rem(lane_slot, slots) == s, seq[s], lane_seq)
        lane_lead = jnp.where(lane_slot == s, lead, lane_lead)
    lane_seq = jnp.where(lane_slot < 3 * slots, lane_seq, -1)
    r = lax.broadcasted_iota(jnp.int32, (nz, hd), 0)
    gather_stat[...] = jnp.where(r == lane_seq, 1.0, 0.0).astype(BF16)

    for s in range(slots):
        loads[s].wait()
        for p in range(pairs):
            ktr[s, p] = kbuf[s, :, p].reshape(wide, hd).T
    for s in range(slots):
        vloads[s].wait()

    row_pass = (mz < reach).astype(jnp.int32)

    def first(b):
        d = jnp.abs(mz - b)
        near = (mz <= middle) | (b < reach) | (jnp.minimum(d, nz - d) <= reach + 1)
        return ((b <= mz) & (mz >= reach) & near).astype(jnp.int32)

    def goes(b, x, late):
        return late == row_pass if b == 0 and x == 0 else first(b) != late

    scale = hd ** -0.5 * math.log2(math.e)

    def one_pass(late, carry):
        for b in range(nz):
            @pl.when((first(b) != late) & ((b != mz) | root))
            def _():
                block_wait(b)

            if b > 0:
                @pl.when(agent)
                def _():
                    block_copy(b, 0, 0, root_send.at[b]).start()

                @pl.when((first(b) != late) & (b != mz))
                def _():
                    q_use[b] = q_land[b]
            else:
                @pl.when(first(b) != late)
                def _():
                    q_use[0, pl.ds(1, nx - 1)] = q_land[0, pl.ds(1, nx - 1)]

        @pl.when(late == row_pass)
        def _():
            @pl.when(~low)
            def _():
                pltpu.make_async_copy(first_row, first_row, root_sem).wait()

            q_use[0, 0] = q_land[0, 0]

        lane = lax.broadcasted_iota(jnp.int32, (rows, wide), 1)
        row = lax.broadcasted_iota(jnp.int32, (rows, wide), 0)
        matched = lax.rem(lane, half) == row // group
        token = jnp.where(matched, lane // half, block)
        left = []
        for b, c in zip(seq, code):
            rest = jnp.clip(lens[b] - lax.rem(c, per_seq) * block, 0, block)
            ours = (first(b) != late) | ((b == 0) & (late == row_pass))
            left.append(jnp.where(ours, rest, 0))
        work = [(p, s) for p in range(pairs) for s in range(slots)]

        def score(p, s):
            q = q_use[seq[s], pl.ds(p * half, half)].reshape(rows, hd)
            return jnp.dot(q, ktr[s, p], preferred_element_type=F32)

        def soften(sc, s):
            live = token < left[s]
            sc = jnp.where(live, sc, NEG)
            m = jnp.max(sc, axis=1, keepdims=True)
            w = jnp.where(live, jnp.exp2((sc - m) * scale), 0.0).astype(BF16)
            return m, jnp.sum(w.astype(F32), axis=1, keepdims=True), w

        peaks, totals, weights, parts = {}, {}, {}, {}
        scores = {}
        for i in range(len(work) + 2):
            if i < len(work):
                scores[i] = score(*work[i])
            if 0 <= i - 1 < len(work):
                peaks[i - 1], totals[i - 1], weights[i - 1] = soften(scores.pop(i - 1), work[i - 1][1])
            if i >= 2:
                p, s = work[i - 2]
                parts[i - 2] = jnp.dot(
                    weights.pop(i - 2), vbuf[s, :, p].reshape(wide, hd), preferred_element_type=F32)
        for p in range(pairs):
            peak, total, part = ([d[p * slots + s] for s in range(slots)] for d in (peaks, totals, parts))
            lane_s = lax.broadcasted_iota(jnp.int32, (rows, hd), 1)
            tops = jnp.full((rows, hd), NEG, F32)
            sums = jnp.zeros((rows, hd), F32)
            best = jnp.full((rows, hd), NEG, F32)
            for s in range(slots):
                tops = jnp.where(lane_s == s, peak[s], tops)
                sums = jnp.where(lane_s == s, total[s], sums)
                best = jnp.maximum(best, jnp.where(lane_seq == seq[s], peak[s], NEG))
            f = jnp.exp2((tops - best) * scale)
            sums = sums * f
            lead = jnp.where(lane_lead == 1, best, 0.0)
            both = jnp.concatenate([part[s] * f[:, s:s + 1] for s in range(slots)], axis=0).astype(BF16)
            acc = jnp.dot(gather[...], both, preferred_element_type=F32)
            for e in range(half):
                half_acc = acc[e * nz * group:(e + 1) * nz * group].reshape(nz, group, hd)
                out_send[late, p * half + e] = half_acc.astype(BF16)
            mixed = []
            for e in range(half):
                mixed += [lead[e * group:(e + 1) * group], sums[e * group:(e + 1) * group]]
            rest = jnp.concatenate(mixed + [jnp.zeros((hd - 2 * rows, hd), F32)], axis=0)
            packed = jnp.zeros((hd, hd), F32)
            for k in range(3):
                coarse = rest.astype(BF16).astype(F32)
                packed = packed + (pltpu.roll(coarse, k * slots, 1) if k else coarse)
                rest = rest - coarse
            st = lax.dot_general(
                gather_stat[...], packed.astype(BF16), (((1,), (1,)), ((), ())), preferred_element_type=F32)
            st_send[late, p] = st.reshape(nz, 1, hd)
        for b in range(nz):
            for x in range(nx):
                @pl.when(goes(b, x, late) & (b * nx + x != me))
                def _():
                    pltpu.make_async_remote_copy(
                        src_ref=out_send.at[late, x, b], dst_ref=out_recv.at[me],
                        send_sem=o_send_sem, recv_sem=o_recv_sem,
                        device_id=at(b, x), device_id_type=MESH).start()
                    pltpu.make_async_remote_copy(
                        src_ref=st_send.at[late, x // half, b], dst_ref=st_recv.at[me],
                        send_sem=s_send_sem, recv_sem=s_recv_sem,
                        device_id=at(b, x), device_id_type=MESH).start()
        return carry

    lax.fori_loop((mz < reach).astype(jnp.int32), 2, one_pass, 0)
    last = (mz < reach).astype(jnp.int32)
    out_recv[me] = out_send[last, mx, mz]
    st_recv[me] = st_send[last, mx // half, mz]
    rest_s = st_recv.at[pl.ds(0, n - 1)]
    rest_o = out_recv.at[pl.ds(0, n - 1)]
    @pl.when(low & ~root)
    def _():
        pltpu.make_async_copy(two, two, x_send_sem).wait()

    @pl.when(root | ~low)
    def _():
        pltpu.make_async_copy(three, three, x_send_sem).wait()

    for z in range(nz):
        @pl.when(~low & (z != mz) & (((z < mz) & ((mx > 0) | (z > 0))) | (z > mz)))
        def _():
            block_copy(mz, z, mx, block_send.at[z]).wait_send()

        @pl.when(agent)
        def _():
            block_copy(z, 0, 0, root_send.at[z]).wait_send()

        if z > 0:
            @pl.when(low & ~root)
            def _():
                row_copy(first_row, z, mx, row_send.at[z], root_sem).wait_send()

            @pl.when(agent)
            def _():
                row_copy(first_row, z, 0, row_send_low.at[z], root_sem).wait_send()

            @pl.when(low & ~root)
            def _():
                block_copy(0, z, mx, block_send.at[z]).wait_send()

            @pl.when(agent)
            def _():
                block_copy(0, z, 0, col_send.at[z]).wait_send()

    pltpu.make_async_copy(rest_o, rest_o, o_send_sem).wait()
    pltpu.make_async_copy(rest_s, rest_s, s_send_sem).wait()
    pltpu.make_async_copy(rest_s, rest_s, s_recv_sem).wait()
    pltpu.make_async_copy(rest_o, rest_o, o_recv_sem).wait()

    stat = st_recv[...].reshape(n, hd)
    stat = jnp.where(lax.rem(mx, half) == 1, pltpu.roll(stat, hd - 2 * group, 1), stat)
    total = pltpu.roll(stat, hd - group, 1)
    stat = jnp.where(total > 0.0, stat, NEG)
    best = jnp.max(stat, axis=0, keepdims=True)
    f = jnp.exp2((stat - best) * scale)
    f = f / jnp.sum(f * total, axis=0, keepdims=True)
    r = lax.broadcasted_iota(jnp.int32, (group, hd), 0)
    c = lax.broadcasted_iota(jnp.int32, (group, hd), 1)
    acc = jnp.zeros((group, hd), F32)
    for i in range(n):
        g = jnp.where(c == r, jnp.broadcast_to(f[i:i + 1], (group, hd)), 0.0)
        acc = acc + jnp.sum(g, axis=1, keepdims=True) * out_recv[i].astype(F32)
    o_ref[...] = acc.astype(BF16)


def solution(mesh):
    n = mesh.shape["seq"]

    def body(queries, keys, values, lengths, slot_block):
        share, _, hd = queries.shape
        slots, block, kv_local, _ = keys.shape
        nz = lengths.shape[0]
        nx = n // nz
        half = 2
        group = share
        split = (slots, block, nx // half, half, hd)
        any_ = pl.BlockSpec(memory_space=pl.ANY)
        dims = (nz, nx, slots, block, group, hd)
        dma, regular = pltpu.SemaphoreType.DMA, pltpu.SemaphoreType.REGULAR
        out = pl.pallas_call(
            functools.partial(attend, dims),
            out_shape=jax.ShapeDtypeStruct((share, hd), BF16),
            in_specs=[any_] * 5,
            out_specs=pl.BlockSpec(memory_space=pltpu.VMEM),
            scratch_shapes=[
                pltpu.VMEM(split, BF16), pltpu.VMEM(split, BF16),
                pltpu.VMEM((slots, nx // half, hd, block * half), BF16),
                pltpu.VMEM((nz * half * share, slots * half * share), BF16),
                pltpu.VMEM((nz, hd), BF16),
                pltpu.VMEM((nz, nx, share, hd), BF16), pltpu.VMEM((nz, nx, share, hd), BF16),
                pltpu.SMEM((nz,), jnp.int32), pltpu.SMEM((slots,), jnp.int32),
                pltpu.VMEM((2, nx, nz, share, hd), BF16), pltpu.VMEM((n, share, hd), BF16),
                pltpu.VMEM((2, nx // half, nz, 1, hd), F32), pltpu.VMEM((n, 1, hd), F32),
                dma((slots,)), dma((slots,)), dma((3,)), regular((nz,)), regular((nz,)), regular((nx,)), dma, dma((nz,)), dma((nz,)), dma((nz,)), dma((nz,)), dma, dma,
                dma((nz,)), dma((nz,)), dma, dma, dma, dma,
            ],
            compiler_params=pltpu.CompilerParams(collective_id=0, has_side_effects=True),
        )(queries.reshape(share, hd), keys.reshape(split), values.reshape(split), lengths, slot_block)
        return out.reshape(share, 1, hd)

    placed = (
        P(("grp", "seq"), "head", None),
        P(("grp", "seq"), None, "head", None),
        P(("grp", "seq"), None, "head", None),
        P("grp"),
        P(("grp", "seq")),
    )
    return jax.shard_map(
        body, mesh=mesh, in_specs=placed, out_specs=P(("grp", "seq"), "head", None), check_vma=False
    )
```

```python
import functools
import math

import jax
import jax.numpy as jnp
from jax import lax
from jax.experimental import pallas as pl
from jax.experimental.pallas import tpu as pltpu
from jax.sharding import PartitionSpec as P

MESH = pl.DeviceIdType.MESH
F32 = jnp.float32
BF16 = jnp.bfloat16
NEG = -1e30


def attend(dims, q_hbm, k_hbm, v_hbm, len_hbm, slot_hbm, o_hbm,
           kbuf, vbuf, ktr, gather, gather_stat, final, q_land, q_use, lens, slot, out_send, out_recv, st_send, st_recv,
           ksem, vsem, small_sem, ready, ready_low, x_ready, root_sem, row_send, row_send_low, root_send, col_send, x_send_sem, x_recv_sem, block_send, block_sem,
           o_send_sem, o_recv_sem, s_send_sem, s_recv_sem):
    nz, nx, slots, block, group, hd = dims
    n = nz * nx
    half = 2
    pairs = nx // half
    rows = half * group
    wide = block * half
    me = lax.axis_index("seq")
    mz, mx = me // nx, lax.rem(me, nx)
    top_z = nz - 1

    reach = nz // 4
    middle = nz // 2

    def at(z, x):
        return {"seq": z * nx + x}

    low = mz == 0
    root = me == 0
    agent = me == 1

    barrier = pltpu.get_barrier_semaphore()

    def greet(z, x):
        pl.semaphore_signal(barrier, inc=1, device_id=at(z, x), device_id_type=MESH)

    for z in range(top_z, 0, -1):
        @pl.when((z > mz) & ~root)
        def _():
            greet(z, mx)

        @pl.when(agent)
        def _():
            greet(z, 0)

    for x in range(nx):
        @pl.when(((x > mx) & ~root) | ((x == 0) & low & ~root))
        def _():
            greet(mz, x)

    own = pltpu.make_async_copy(q_hbm, q_land.at[mz, mx], small_sem.at[2])
    own.start()

    @pl.when(root)
    def _():
        pl.semaphore_wait(barrier, nx - 1)

    @pl.when(me > 1)
    def _():
        pl.semaphore_wait(barrier, mz + mx - low.astype(jnp.int32))

    for z in range(top_z):
        @pl.when((z < mz) & ((mx > 0) | (z > 0)))
        def _():
            pl.semaphore_signal(ready.at[mz], inc=1, device_id=at(z, mx), device_id_type=MESH)

    @pl.when((mx == 0) & ~low)
    def _():
        pl.semaphore_signal(ready_low.at[mz], inc=1, device_id=at(0, 1), device_id_type=MESH)

    for x in range(nx - 1):
        @pl.when((x < mx) & ((x > 0) | ~low))
        def _():
            pl.semaphore_signal(x_ready.at[mx], inc=1, device_id=at(mz, x), device_id_type=MESH)

    small = [
        pltpu.make_async_copy(slot_hbm, slot, small_sem.at[0]),
        pltpu.make_async_copy(len_hbm, lens, small_sem.at[1]),
    ]
    loads = [pltpu.make_async_copy(k_hbm.at[s], kbuf.at[s], ksem.at[s]) for s in range(slots)]
    vloads = [pltpu.make_async_copy(v_hbm.at[s], vbuf.at[s], vsem.at[s]) for s in range(slots)]
    for c in small + loads + vloads:
        c.start()
    own.wait()
    first_row = q_land.at[0, 0]

    def row_copy(row, z, x, send, recv):
        return pltpu.make_async_remote_copy(
            src_ref=row, dst_ref=row, send_sem=send, recv_sem=recv, device_id=at(z, x), device_id_type=MESH)

    for x in range(nx):
        @pl.when((x > mx) & ~root)
        def _():
            pl.semaphore_wait(x_ready.at[x], 1)

        @pl.when((x != mx) & ((x > 0) | ~low) & ~root)
        def _():
            row_copy(q_land.at[mz, mx], mz, x, x_send_sem, x_recv_sem).start()

        @pl.when((x > 0) & root)
        def _():
            row_copy(first_row, 0, x, x_send_sem, root_sem).start()

    three = q_land.at[mz, pl.ds(0, nx - 1)]
    two = q_land.at[mz, pl.ds(0, nx - 2)]

    def piece(b):
        return q_land.at[0, pl.ds(1, nx - 1)] if isinstance(b, int) and b == 0 else q_land.at[b]

    def block_copy(b, z, x, sem):
        return row_copy(piece(b), z, x, sem, block_sem.at[b])

    def block_wait(b):
        pltpu.make_async_copy(piece(b), piece(b), block_sem.at[b]).wait()

    q_use[0, 0] = jnp.zeros((group, hd), BF16)

    @pl.when(low & ~root)
    def _():
        pltpu.make_async_copy(two, two, x_recv_sem).wait()

    @pl.when(~low)
    def _():
        pltpu.make_async_copy(three, three, x_recv_sem).wait()
        q_use[mz] = q_land[mz]

    for b in range(top_z):
        @pl.when((b < mz) & ((mx > 0) | (b > 0)))
        def _():
            block_copy(mz, b, mx, block_send.at[b]).start()

    def send_row(z):
        @pl.when(low & ~root)
        def _():
            row_copy(first_row, z, mx, row_send.at[z], root_sem).start()

        @pl.when(agent)
        def _():
            row_copy(first_row, z, 0, row_send_low.at[z], root_sem).start()

    for z in range(1, nz):
        if z == middle:
            @pl.when(low & ~root)
            def _():
                pltpu.make_async_copy(first_row, first_row, root_sem).wait()

        @pl.when((z > mz) & ~root)
        def _():
            pl.semaphore_wait(ready.at[z], 1)

            @pl.when(~low)
            def _():
                block_copy(mz, z, mx, block_send.at[z]).start()

            @pl.when(low)
            def _():
                block_copy(0, z, mx, block_send.at[z]).start()

        @pl.when(agent)
        def _():
            pl.semaphore_wait(ready_low.at[z], 1)
            block_copy(0, z, 0, col_send.at[z]).start()

        if z >= middle:
            send_row(z)

    for z in range(1, middle):
        send_row(z)

    @pl.when(agent)
    def _():
        block_copy(0, 0, 0, root_send.at[0]).start()

    for c in small:
        c.wait()
    per_seq = slots * n // nz
    code = [slot[s] for s in range(slots)]
    seq = [c // per_seq for c in code]
    col = lax.broadcasted_iota(jnp.int32, (1, slots * rows), 1)
    seq_at = jnp.zeros_like(col)
    for s in range(slots):
        seq_at = jnp.where(col // rows == s, seq[s], seq_at)
    r = lax.broadcasted_iota(jnp.int32, (nz * rows, slots * rows), 0)
    c = lax.broadcasted_iota(jnp.int32, (nz * rows, slots * rows), 1)
    wanted = r // (nz * group) * group + lax.rem(r, group)
    same = (lax.rem(r, nz * group) // group == seq_at) & (wanted == lax.rem(c, rows))
    gather[...] = jnp.where(same, 1.0, 0.0).astype(BF16)
    lane_slot = lax.broadcasted_iota(jnp.int32, (1, hd), 1)
    lane_seq = jnp.full((1, hd), -1, jnp.int32)
    lane_lead = jnp.zeros((1, hd), jnp.int32)
    for s in range(slots):
        lead = 1
        for t in range(s):
            lead = lead * (seq[t] != seq[s]).astype(jnp.int32)
        lane_seq = jnp.where(lax.rem(lane_slot, slots) == s, seq[s], lane_seq)
        lane_lead = jnp.where(lane_slot == s, lead, lane_lead)
    lane_seq = jnp.where(lane_slot < 3 * slots, lane_seq, -1)
    r = lax.broadcasted_iota(jnp.int32, (nz, hd), 0)
    gather_stat[...] = jnp.where(r == lane_seq, 1.0, 0.0).astype(BF16)

    for s in range(slots):
        loads[s].wait()
        for p in range(pairs):
            ktr[s, p] = kbuf[s, :, p].reshape(wide, hd).T
    for s in range(slots):
        vloads[s].wait()

    row_pass = (mz < reach).astype(jnp.int32)

    def first(b):
        d = jnp.abs(mz - b)
        near = (mz <= middle) | (b <= reach) | (jnp.minimum(d, nz - d) <= reach + 1)
        return ((b <= mz) & (mz >= reach) & near).astype(jnp.int32)

    def goes(b, x, late):
        return late == row_pass if b == 0 and x == 0 else first(b) != late

    scale = hd ** -0.5 * math.log2(math.e)

    def one_pass(late, carry):
        for b in range(nz):
            @pl.when((first(b) != late) & ((b != mz) | root))
            def _():
                block_wait(b)

            if b > 0:
                @pl.when(agent)
                def _():
                    block_copy(b, 0, 0, root_send.at[b]).start()

                @pl.when((first(b) != late) & (b != mz))
                def _():
                    q_use[b] = q_land[b]
            else:
                @pl.when(first(b) != late)
                def _():
                    q_use[0, pl.ds(1, nx - 1)] = q_land[0, pl.ds(1, nx - 1)]

        @pl.when(late == row_pass)
        def _():
            @pl.when(~low)
            def _():
                pltpu.make_async_copy(first_row, first_row, root_sem).wait()

            q_use[0, 0] = q_land[0, 0]

        lane = lax.broadcasted_iota(jnp.int32, (rows, wide), 1)
        row = lax.broadcasted_iota(jnp.int32, (rows, wide), 0)
        matched = lax.rem(lane, half) == row // group
        token = jnp.where(matched, lane // half, block)
        left = []
        for b, c in zip(seq, code):
            rest = jnp.clip(lens[b] - lax.rem(c, per_seq) * block, 0, block)
            ours = (first(b) != late) | ((b == 0) & (late == row_pass))
            left.append(jnp.where(ours, rest, 0))
        work = [(p, s) for p in range(pairs) for s in range(slots)]

        def score(p, s):
            q = q_use[seq[s], pl.ds(p * half, half)].reshape(rows, hd)
            return jnp.dot(q, ktr[s, p], preferred_element_type=F32)

        def soften(sc, s):
            live = token < left[s]
            sc = jnp.where(live, sc, NEG)
            m = jnp.max(sc, axis=1, keepdims=True)
            w = jnp.where(live, jnp.exp2((sc - m) * scale), 0.0).astype(BF16)
            return m, jnp.sum(w.astype(F32), axis=1, keepdims=True), w

        peaks, totals, weights, parts = {}, {}, {}, {}
        scores = {}
        for i in range(len(work) + 2):
            if i < len(work):
                scores[i] = score(*work[i])
            if 0 <= i - 1 < len(work):
                peaks[i - 1], totals[i - 1], weights[i - 1] = soften(scores.pop(i - 1), work[i - 1][1])
            if i >= 2:
                p, s = work[i - 2]
                parts[i - 2] = jnp.dot(
                    weights.pop(i - 2), vbuf[s, :, p].reshape(wide, hd), preferred_element_type=F32)
        for p in range(pairs):
            peak, total, part = ([d[p * slots + s] for s in range(slots)] for d in (peaks, totals, parts))
            lane_s = lax.broadcasted_iota(jnp.int32, (rows, hd), 1)
            tops = jnp.full((rows, hd), NEG, F32)
            sums = jnp.zeros((rows, hd), F32)
            best = jnp.full((rows, hd), NEG, F32)
            for s in range(slots):
                tops = jnp.where(lane_s == s, peak[s], tops)
                sums = jnp.where(lane_s == s, total[s], sums)
                best = jnp.maximum(best, jnp.where(lane_seq == seq[s], peak[s], NEG))
            f = jnp.exp2((tops - best) * scale)
            sums = sums * f
            lead = jnp.where(lane_lead == 1, best, 0.0)
            both = jnp.concatenate([part[s] * f[:, s:s + 1] for s in range(slots)], axis=0).astype(BF16)
            acc = jnp.dot(gather[...], both, preferred_element_type=F32)
            for e in range(half):
                half_acc = acc[e * nz * group:(e + 1) * nz * group].reshape(nz, group, hd)
                out_send[late, p * half + e] = half_acc.astype(BF16)
            mixed = []
            for e in range(half):
                mixed += [lead[e * group:(e + 1) * group], sums[e * group:(e + 1) * group]]
            rest = jnp.concatenate(mixed + [jnp.zeros((hd - 2 * rows, hd), F32)], axis=0)
            packed = jnp.zeros((hd, hd), F32)
            for k in range(3):
                coarse = rest.astype(BF16).astype(F32)
                packed = packed + (pltpu.roll(coarse, k * slots, 1) if k else coarse)
                rest = rest - coarse
            st = lax.dot_general(
                gather_stat[...], packed.astype(BF16), (((1,), (1,)), ((), ())), preferred_element_type=F32)
            st_send[late, p] = st.reshape(nz, 1, hd)
        for b in range(nz):
            for x in range(nx):
                @pl.when(goes(b, x, late) & (b * nx + x != me))
                def _():
                    pltpu.make_async_remote_copy(
                        src_ref=out_send.at[late, x, b], dst_ref=out_recv.at[me],
                        send_sem=o_send_sem, recv_sem=o_recv_sem,
                        device_id=at(b, x), device_id_type=MESH).start()
                    pltpu.make_async_remote_copy(
                        src_ref=st_send.at[late, x // half, b], dst_ref=st_recv.at[me],
                        send_sem=s_send_sem, recv_sem=s_recv_sem,
                        device_id=at(b, x), device_id_type=MESH).start()
        return carry

    lax.fori_loop((mz < reach).astype(jnp.int32), 2, one_pass, 0)
    last = (mz < reach).astype(jnp.int32)
    out_recv[me] = out_send[last, mx, mz]
    st_recv[me] = st_send[last, mx // half, mz]
    rest_s = st_recv.at[pl.ds(0, n - 1)]
    rest_o = out_recv.at[pl.ds(0, n - 1)]
    @pl.when(low & ~root)
    def _():
        pltpu.make_async_copy(two, two, x_send_sem).wait()

    @pl.when(root | ~low)
    def _():
        pltpu.make_async_copy(three, three, x_send_sem).wait()

    for z in range(nz):
        @pl.when(~low & (z != mz) & (((z < mz) & ((mx > 0) | (z > 0))) | (z > mz)))
        def _():
            block_copy(mz, z, mx, block_send.at[z]).wait_send()

        @pl.when(agent)
        def _():
            block_copy(z, 0, 0, root_send.at[z]).wait_send()

        if z > 0:
            @pl.when(low & ~root)
            def _():
                row_copy(first_row, z, mx, row_send.at[z], root_sem).wait_send()

            @pl.when(agent)
            def _():
                row_copy(first_row, z, 0, row_send_low.at[z], root_sem).wait_send()

            @pl.when(low & ~root)
            def _():
                block_copy(0, z, mx, block_send.at[z]).wait_send()

            @pl.when(agent)
            def _():
                block_copy(0, z, 0, col_send.at[z]).wait_send()

    pltpu.make_async_copy(rest_o, rest_o, o_send_sem).wait()
    pltpu.make_async_copy(rest_s, rest_s, s_send_sem).wait()
    pltpu.make_async_copy(rest_s, rest_s, s_recv_sem).wait()
    pltpu.make_async_copy(rest_o, rest_o, o_recv_sem).wait()

    stat = st_recv[...].reshape(n, hd)
    stat = jnp.where(lax.rem(mx, half) == 1, pltpu.roll(stat, hd - 2 * group, 1), stat)
    total = pltpu.roll(stat, hd - group, 1)
    stat = jnp.where(total > 0.0, stat, NEG)
    best = jnp.max(stat, axis=0, keepdims=True)
    f = jnp.exp2((stat - best) * scale)
    f = f / jnp.sum(f * total, axis=0, keepdims=True)
    r = lax.broadcasted_iota(jnp.int32, (group, hd), 0)
    c = lax.broadcasted_iota(jnp.int32, (group, hd), 1)
    acc = jnp.zeros((group, hd), F32)
    for i in range(n):
        g = jnp.where(c == r, jnp.broadcast_to(f[i:i + 1], (group, hd)), 0.0)
        acc = acc + jnp.sum(g, axis=1, keepdims=True) * out_recv[i].astype(F32)
    final[...] = acc.astype(BF16)
    out = pltpu.make_async_copy(final, o_hbm, small_sem.at[2])
    out.start()
    out.wait()


def solution(mesh):
    n = mesh.shape["seq"]

    def body(queries, keys, values, lengths, slot_block):
        share, _, hd = queries.shape
        slots, block, kv_local, _ = keys.shape
        nz = lengths.shape[0]
        nx = n // nz
        half = 2
        group = share
        split = (slots, block, nx // half, half, hd)
        any_ = pl.BlockSpec(memory_space=pl.ANY)
        dims = (nz, nx, slots, block, group, hd)
        dma, regular = pltpu.SemaphoreType.DMA, pltpu.SemaphoreType.REGULAR
        out = pl.pallas_call(
            functools.partial(attend, dims),
            out_shape=jax.ShapeDtypeStruct((share, hd), BF16),
            in_specs=[any_] * 5,
            out_specs=any_,
            scratch_shapes=[
                pltpu.VMEM(split, BF16), pltpu.VMEM(split, BF16),
                pltpu.VMEM((slots, nx // half, hd, block * half), BF16),
                pltpu.VMEM((nz * half * share, slots * half * share), BF16),
                pltpu.VMEM((nz, hd), BF16), pltpu.VMEM((share, hd), BF16),
                pltpu.VMEM((nz, nx, share, hd), BF16), pltpu.VMEM((nz, nx, share, hd), BF16),
                pltpu.SMEM((nz,), jnp.int32), pltpu.SMEM((slots,), jnp.int32),
                pltpu.VMEM((2, nx, nz, share, hd), BF16), pltpu.VMEM((n, share, hd), BF16),
                pltpu.VMEM((2, nx // half, nz, 1, hd), F32), pltpu.VMEM((n, 1, hd), F32),
                dma((slots,)), dma((slots,)), dma((3,)), regular((nz,)), regular((nz,)), regular((nx,)), dma, dma((nz,)), dma((nz,)), dma((nz,)), dma((nz,)), dma, dma,
                dma((nz,)), dma((nz,)), dma, dma, dma, dma,
            ],
            compiler_params=pltpu.CompilerParams(collective_id=0, has_side_effects=True),
        )(queries.reshape(share, hd), keys.reshape(split), values.reshape(split), lengths, slot_block)
        return out.reshape(share, 1, hd)

    placed = (
        P(("grp", "seq"), "head", None),
        P(("grp", "seq"), None, "head", None),
        P(("grp", "seq"), None, "head", None),
        P("grp"),
        P(("grp", "seq")),
    )
    return jax.shard_map(
        body, mesh=mesh, in_specs=placed, out_specs=P(("grp", "seq"), "head", None), check_vma=False
    )
```

```python
import functools
import math

import jax
import jax.numpy as jnp
from jax import lax
from jax.experimental import pallas as pl
from jax.experimental.pallas import tpu as pltpu
from jax.sharding import PartitionSpec as P

MESH = pl.DeviceIdType.MESH
F32 = jnp.float32
BF16 = jnp.bfloat16
NEG = -1e30


def attend(dims, q_hbm, k_hbm, v_hbm, len_hbm, slot_hbm, o_hbm,
           kbuf, vbuf, ktr, gather, gather_stat, final, q_land, q_use, lens, slot, out_send, out_recv, st_send, st_recv,
           ksem, vsem, small_sem, ready, ready_low, x_ready, root_sem, row_send, root_send, col_send, x_send_sem, x_recv_sem, block_send, block_sem,
           o_send_sem, o_recv_sem, s_send_sem, s_recv_sem):
    nz, nx, slots, block, group, hd = dims
    n = nz * nx
    half = 2
    pairs = nx // half
    rows = half * group
    wide = block * half
    me = lax.axis_index("seq")
    mz, mx = me // nx, lax.rem(me, nx)
    top_z = nz - 1

    reach = nz // 4
    middle = nz // 2

    def at(z, x):
        return {"seq": z * nx + x}

    low = mz == 0
    root = me == 0
    agent = me == 1

    barrier = pltpu.get_barrier_semaphore()

    def greet(z, x):
        pl.semaphore_signal(barrier, inc=1, device_id=at(z, x), device_id_type=MESH)

    for z in range(top_z, 0, -1):
        @pl.when((z > mz) & ~root)
        def _():
            greet(z, mx)

        @pl.when(agent)
        def _():
            greet(z, 0)

    for x in range(nx):
        @pl.when(((x > mx) & ~root) | ((x == 0) & low & ~root))
        def _():
            greet(mz, x)

    own = pltpu.make_async_copy(q_hbm, q_land.at[mz, mx], small_sem.at[2])
    own.start()

    @pl.when(root)
    def _():
        pl.semaphore_wait(barrier, nx - 1)

    @pl.when(me > 1)
    def _():
        pl.semaphore_wait(barrier, mz + mx - low.astype(jnp.int32))

    for z in range(top_z):
        @pl.when((z < mz) & ((mx > 0) | (z > 0)))
        def _():
            pl.semaphore_signal(ready.at[mz], inc=1, device_id=at(z, mx), device_id_type=MESH)

    @pl.when((mx == 0) & ~low)
    def _():
        pl.semaphore_signal(ready_low.at[mz], inc=1, device_id=at(0, 1), device_id_type=MESH)

    for x in range(nx - 1):
        @pl.when((x < mx) & ((x > 0) | ~low))
        def _():
            pl.semaphore_signal(x_ready.at[mx], inc=1, device_id=at(mz, x), device_id_type=MESH)

    small = [
        pltpu.make_async_copy(slot_hbm, slot, small_sem.at[0]),
        pltpu.make_async_copy(len_hbm, lens, small_sem.at[1]),
    ]
    loads = [pltpu.make_async_copy(k_hbm.at[s], kbuf.at[s], ksem) for s in range(slots)]
    vloads = [pltpu.make_async_copy(v_hbm.at[s], vbuf.at[s], vsem) for s in range(slots)]
    for c in small + loads + vloads:
        c.start()
    own.wait()
    first_row = q_land.at[0, 0]

    def row_copy(row, z, x, send, recv):
        return pltpu.make_async_remote_copy(
            src_ref=row, dst_ref=row, send_sem=send, recv_sem=recv, device_id=at(z, x), device_id_type=MESH)

    for x in range(nx):
        @pl.when((x > mx) & ~root)
        def _():
            pl.semaphore_wait(x_ready.at[x], 1)

        @pl.when((x != mx) & ((x > 0) | ~low) & ~root)
        def _():
            row_copy(q_land.at[mz, mx], mz, x, x_send_sem, x_recv_sem).start()

        @pl.when((x > 0) & root)
        def _():
            row_copy(first_row, 0, x, x_send_sem, root_sem).start()

    three = q_land.at[mz, pl.ds(0, nx - 1)]
    two = q_land.at[mz, pl.ds(0, nx - 2)]

    def piece(b):
        return q_land.at[0, pl.ds(1, nx - 1)] if isinstance(b, int) and b == 0 else q_land.at[b]

    def block_copy(b, z, x, sem):
        return row_copy(piece(b), z, x, sem, block_sem.at[b])

    def block_wait(b):
        pltpu.make_async_copy(piece(b), piece(b), block_sem.at[b]).wait()

    q_use[0, 0] = jnp.zeros((group, hd), BF16)

    @pl.when(low & ~root)
    def _():
        pltpu.make_async_copy(two, two, x_recv_sem).wait()

    @pl.when(~low)
    def _():
        pltpu.make_async_copy(three, three, x_recv_sem).wait()
        q_use[mz] = q_land[mz]

    for b in range(top_z):
        @pl.when((b < mz) & ((mx > 0) | (b > 0)))
        def _():
            block_copy(mz, b, mx, block_send).start()

    def send_row(z):
        @pl.when(low & ~root)
        def _():
            row_copy(first_row, z, mx, row_send, root_sem).start()

        @pl.when(agent)
        def _():
            row_copy(first_row, z, 0, row_send, root_sem).start()

    for z in range(1, nz):
        if z == middle:
            @pl.when(low & ~root)
            def _():
                pltpu.make_async_copy(first_row, first_row, root_sem).wait()

        @pl.when((z > mz) & ~root)
        def _():
            pl.semaphore_wait(ready.at[z], 1)

            @pl.when(~low)
            def _():
                block_copy(mz, z, mx, block_send).start()

            @pl.when(low)
            def _():
                block_copy(0, z, mx, block_send).start()

        @pl.when(agent)
        def _():
            pl.semaphore_wait(ready_low.at[z], 1)
            block_copy(0, z, 0, col_send).start()

        if z >= middle:
            send_row(z)

    for z in range(1, middle):
        send_row(z)

    @pl.when(agent)
    def _():
        block_copy(0, 0, 0, root_send).start()

    for c in small:
        c.wait()
    per_seq = slots * n // nz
    code = [slot[s] for s in range(slots)]
    seq = [c // per_seq for c in code]
    col = lax.broadcasted_iota(jnp.int32, (1, slots * rows), 1)
    seq_at = jnp.zeros_like(col)
    for s in range(slots):
        seq_at = jnp.where(col // rows == s, seq[s], seq_at)
    r = lax.broadcasted_iota(jnp.int32, (nz * rows, slots * rows), 0)
    c = lax.broadcasted_iota(jnp.int32, (nz * rows, slots * rows), 1)
    wanted = r // (nz * group) * group + lax.rem(r, group)
    same = (lax.rem(r, nz * group) // group == seq_at) & (wanted == lax.rem(c, rows))
    gather[...] = jnp.where(same, 1.0, 0.0).astype(BF16)
    lane_slot = lax.broadcasted_iota(jnp.int32, (1, hd), 1)
    lane_seq = jnp.full((1, hd), -1, jnp.int32)
    lane_lead = jnp.zeros((1, hd), jnp.int32)
    for s in range(slots):
        lead = 1
        for t in range(s):
            lead = lead * (seq[t] != seq[s]).astype(jnp.int32)
        lane_seq = jnp.where(lax.rem(lane_slot, slots) == s, seq[s], lane_seq)
        lane_lead = jnp.where(lane_slot == s, lead, lane_lead)
    lane_seq = jnp.where(lane_slot < 3 * slots, lane_seq, -1)
    r = lax.broadcasted_iota(jnp.int32, (nz, hd), 0)
    gather_stat[...] = jnp.where(r == lane_seq, 1.0, 0.0).astype(BF16)

    pltpu.make_async_copy(k_hbm, kbuf, ksem).wait()
    for s in range(slots):
        for p in range(pairs):
            ktr[s, p] = kbuf[s, :, p].reshape(wide, hd).T
    pltpu.make_async_copy(v_hbm, vbuf, vsem).wait()

    row_pass = (mz < reach).astype(jnp.int32)

    def first(b):
        d = jnp.abs(mz - b)
        near = (mz <= middle) | (b < reach) | (jnp.minimum(d, nz - d) <= reach + 1)
        return ((b <= mz) & (mz >= reach) & near).astype(jnp.int32)

    def goes(b, x, late):
        return late == row_pass if b == 0 and x == 0 else first(b) != late

    scale = hd ** -0.5 * math.log2(math.e)

    def one_pass(late, carry):
        for b in range(nz):
            @pl.when((first(b) != late) & ((b != mz) | root))
            def _():
                block_wait(b)

            if b > 0:
                @pl.when(agent)
                def _():
                    block_copy(b, 0, 0, root_send).start()

                @pl.when((first(b) != late) & (b != mz))
                def _():
                    q_use[b] = q_land[b]
            else:
                @pl.when(first(b) != late)
                def _():
                    q_use[0, pl.ds(1, nx - 1)] = q_land[0, pl.ds(1, nx - 1)]

        @pl.when(late == row_pass)
        def _():
            @pl.when(~low)
            def _():
                pltpu.make_async_copy(first_row, first_row, root_sem).wait()

            q_use[0, 0] = q_land[0, 0]

        lane = lax.broadcasted_iota(jnp.int32, (rows, wide), 1)
        row = lax.broadcasted_iota(jnp.int32, (rows, wide), 0)
        matched = lax.rem(lane, half) == row // group
        token = jnp.where(matched, lane // half, block)
        left = []
        for b, c in zip(seq, code):
            rest = jnp.clip(lens[b] - lax.rem(c, per_seq) * block, 0, block)
            ours = (first(b) != late) | ((b == 0) & (late == row_pass))
            left.append(jnp.where(ours, rest, 0))
        work = [(p, s) for p in range(pairs) for s in range(slots)]

        def score(p, s):
            q = q_use[seq[s], pl.ds(p * half, half)].reshape(rows, hd)
            return jnp.dot(q, ktr[s, p], preferred_element_type=F32)

        def soften(sc, s):
            live = token < left[s]
            sc = jnp.where(live, sc, NEG)
            m = jnp.max(sc, axis=1, keepdims=True)
            w = jnp.where(live, jnp.exp2((sc - m) * scale), 0.0).astype(BF16)
            return m, jnp.sum(w.astype(F32), axis=1, keepdims=True), w

        peaks, totals, weights, parts = {}, {}, {}, {}
        scores = {}
        for i in range(len(work) + 2):
            if i < len(work):
                scores[i] = score(*work[i])
            if 0 <= i - 1 < len(work):
                peaks[i - 1], totals[i - 1], weights[i - 1] = soften(scores.pop(i - 1), work[i - 1][1])
            if i >= 2:
                p, s = work[i - 2]
                parts[i - 2] = jnp.dot(
                    weights.pop(i - 2), vbuf[s, :, p].reshape(wide, hd), preferred_element_type=F32)
        for p in range(pairs):
            peak, total, part = ([d[p * slots + s] for s in range(slots)] for d in (peaks, totals, parts))
            lane_s = lax.broadcasted_iota(jnp.int32, (rows, hd), 1)
            tops = jnp.full((rows, hd), NEG, F32)
            sums = jnp.zeros((rows, hd), F32)
            best = jnp.full((rows, hd), NEG, F32)
            for s in range(slots):
                tops = jnp.where(lane_s == s, peak[s], tops)
                sums = jnp.where(lane_s == s, total[s], sums)
                best = jnp.maximum(best, jnp.where(lane_seq == seq[s], peak[s], NEG))
            f = jnp.exp2((tops - best) * scale)
            sums = sums * f
            lead = jnp.where(lane_lead == 1, best, 0.0)
            both = jnp.concatenate([part[s] * f[:, s:s + 1] for s in range(slots)], axis=0).astype(BF16)
            acc = jnp.dot(gather[...], both, preferred_element_type=F32)
            for e in range(half):
                half_acc = acc[e * nz * group:(e + 1) * nz * group].reshape(nz, group, hd)
                out_send[late, p * half + e] = half_acc.astype(BF16)
            mixed = []
            for e in range(half):
                mixed += [lead[e * group:(e + 1) * group], sums[e * group:(e + 1) * group]]
            rest = jnp.concatenate(mixed + [jnp.zeros((hd - 2 * rows, hd), F32)], axis=0)
            packed = jnp.zeros((hd, hd), F32)
            for k in range(3):
                coarse = rest.astype(BF16).astype(F32)
                packed = packed + (pltpu.roll(coarse, k * slots, 1) if k else coarse)
                rest = rest - coarse
            st = lax.dot_general(
                gather_stat[...], packed.astype(BF16), (((1,), (1,)), ((), ())), preferred_element_type=F32)
            st_send[late, p] = st.reshape(nz, 1, hd)
        for b in range(nz):
            for x in range(nx):
                @pl.when(goes(b, x, late) & (b * nx + x != me))
                def _():
                    pltpu.make_async_remote_copy(
                        src_ref=out_send.at[late, x, b], dst_ref=out_recv.at[me],
                        send_sem=o_send_sem, recv_sem=o_recv_sem,
                        device_id=at(b, x), device_id_type=MESH).start()
                    pltpu.make_async_remote_copy(
                        src_ref=st_send.at[late, x // half, b], dst_ref=st_recv.at[me],
                        send_sem=s_send_sem, recv_sem=s_recv_sem,
                        device_id=at(b, x), device_id_type=MESH).start()
        return carry

    lax.fori_loop((mz < reach).astype(jnp.int32), 2, one_pass, 0)
    last = (mz < reach).astype(jnp.int32)
    out_recv[me] = out_send[last, mx, mz]
    st_recv[me] = st_send[last, mx // half, mz]
    rest_s = st_recv.at[pl.ds(0, n - 1)]
    rest_o = out_recv.at[pl.ds(0, n - 1)]
    @pl.when(low & ~root)
    def _():
        pltpu.make_async_copy(two, two, x_send_sem).wait()

    @pl.when(root | ~low)
    def _():
        pltpu.make_async_copy(three, three, x_send_sem).wait()

    def sent(sem, count):
        moved = out_recv.at[pl.ds(0, count)]
        pltpu.make_async_copy(moved, moved, sem).wait()

    @pl.when(~low & (mx > 0))
    def _():
        sent(block_send, (nz - 1) * nx)

    @pl.when(~low & (mx == 0))
    def _():
        sent(block_send, (nz - 2) * nx)

    @pl.when(low & ~root)
    def _():
        sent(block_send, (nz - 1) * (nx - 1))

    @pl.when(low & ~root & ~agent)
    def _():
        sent(row_send, nz - 1)

    @pl.when(agent)
    def _():
        sent(row_send, 2 * (nz - 1))
        sent(col_send, (nz - 1) * (nx - 1))
        sent(root_send, n - 1)

    pltpu.make_async_copy(rest_o, rest_o, o_send_sem).wait()
    pltpu.make_async_copy(rest_s, rest_s, s_send_sem).wait()
    pltpu.make_async_copy(rest_s, rest_s, s_recv_sem).wait()
    pltpu.make_async_copy(rest_o, rest_o, o_recv_sem).wait()

    stat = st_recv[...].reshape(n, hd)
    stat = jnp.where(lax.rem(mx, half) == 1, pltpu.roll(stat, hd - 2 * group, 1), stat)
    total = pltpu.roll(stat, hd - group, 1)
    stat = jnp.where(total > 0.0, stat, NEG)
    best = jnp.max(stat, axis=0, keepdims=True)
    f = jnp.exp2((stat - best) * scale)
    f = f / jnp.sum(f * total, axis=0, keepdims=True)
    r = lax.broadcasted_iota(jnp.int32, (group, hd), 0)
    c = lax.broadcasted_iota(jnp.int32, (group, hd), 1)
    acc = jnp.zeros((group, hd), F32)
    for i in range(n):
        g = jnp.where(c == r, jnp.broadcast_to(f[i:i + 1], (group, hd)), 0.0)
        acc = acc + jnp.sum(g, axis=1, keepdims=True) * out_recv[i].astype(F32)
    final[...] = acc.astype(BF16)
    out = pltpu.make_async_copy(final, o_hbm, small_sem.at[2])
    out.start()
    out.wait()


def solution(mesh):
    n = mesh.shape["seq"]

    def body(queries, keys, values, lengths, slot_block):
        share, _, hd = queries.shape
        slots, block, kv_local, _ = keys.shape
        nz = lengths.shape[0]
        nx = n // nz
        half = 2
        group = share
        split = (slots, block, nx // half, half, hd)
        any_ = pl.BlockSpec(memory_space=pl.ANY)
        dims = (nz, nx, slots, block, group, hd)
        dma, regular = pltpu.SemaphoreType.DMA, pltpu.SemaphoreType.REGULAR
        out = pl.pallas_call(
            functools.partial(attend, dims),
            out_shape=jax.ShapeDtypeStruct((share, hd), BF16),
            in_specs=[any_] * 5,
            out_specs=any_,
            scratch_shapes=[
                pltpu.VMEM(split, BF16), pltpu.VMEM(split, BF16),
                pltpu.VMEM((slots, nx // half, hd, block * half), BF16),
                pltpu.VMEM((nz * half * share, slots * half * share), BF16),
                pltpu.VMEM((nz, hd), BF16), pltpu.VMEM((share, hd), BF16),
                pltpu.VMEM((nz, nx, share, hd), BF16), pltpu.VMEM((nz, nx, share, hd), BF16),
                pltpu.SMEM((nz,), jnp.int32), pltpu.SMEM((slots,), jnp.int32),
                pltpu.VMEM((2, nx, nz, share, hd), BF16), pltpu.VMEM((n, share, hd), BF16),
                pltpu.VMEM((2, nx // half, nz, 1, hd), F32), pltpu.VMEM((n, 1, hd), F32),
                dma, dma, dma((3,)), regular((nz,)), regular((nz,)), regular((nx,)), dma, dma, dma, dma,
                dma, dma, dma, dma((nz,)), dma, dma, dma, dma,
            ],
            compiler_params=pltpu.CompilerParams(collective_id=0, has_side_effects=True),
        )(queries.reshape(share, hd), keys.reshape(split), values.reshape(split), lengths, slot_block)
        return out.reshape(share, 1, hd)

    placed = (
        P(("grp", "seq"), "head", None),
        P(("grp", "seq"), None, "head", None),
        P(("grp", "seq"), None, "head", None),
        P("grp"),
        P(("grp", "seq")),
    )
    return jax.shard_map(
        body, mesh=mesh, in_specs=placed, out_specs=P(("grp", "seq"), "head", None), check_vma=False
    )
```

```python
import functools
import math

import jax
import jax.numpy as jnp
from jax import lax
from jax.experimental import pallas as pl
from jax.experimental.pallas import tpu as pltpu
from jax.sharding import PartitionSpec as P

MESH = pl.DeviceIdType.MESH
F32 = jnp.float32
BF16 = jnp.bfloat16
NEG = -1e30


def attend(dims, q_hbm, k_hbm, v_hbm, len_hbm, slot_hbm, o_hbm,
           kbuf, vbuf, ktr, gather, gather_stat, final, q_land, q_use, lens, slot, out_send, out_recv, st_send, st_recv,
           ksem, vsem, small_sem, ready, x_ready, root_sem, row_send, root_send, col_send, x_send_sem, x_recv_sem, block_send, block_sem,
           o_send_sem, o_recv_sem, s_send_sem, s_recv_sem):
    nz, nx, slots, block, group, hd = dims
    n = nz * nx
    half = 2
    pairs = nx // half
    rows = half * group
    wide = block * half
    me = lax.axis_index("seq")
    mz, mx = me // nx, lax.rem(me, nx)
    top_z = nz - 1

    reach = nz // 4
    middle = nz // 2

    def at(z, x):
        return {"seq": z * nx + x}

    low = mz == 0
    root = me == 0
    agent = me == 1

    barrier = pltpu.get_barrier_semaphore()

    def greet(z, x):
        pl.semaphore_signal(barrier, inc=1, device_id=at(z, x), device_id_type=MESH)

    for z in range(top_z, 0, -1):
        @pl.when((z > mz) & ~root)
        def _():
            greet(z, mx)

        @pl.when(agent)
        def _():
            greet(z, 0)

    for x in range(nx):
        @pl.when(((x > mx) & ~root) | ((x == 0) & low & ~root))
        def _():
            greet(mz, x)

    own = pltpu.make_async_copy(q_hbm, q_land.at[mz, mx], small_sem.at[2])
    own.start()

    @pl.when(root)
    def _():
        pl.semaphore_wait(barrier, nx - 1)

    @pl.when(me > 1)
    def _():
        pl.semaphore_wait(barrier, mz + mx - low.astype(jnp.int32))

    for z in range(top_z):
        @pl.when((z < mz) & ((mx > 0) | (z > 0)))
        def _():
            pl.semaphore_signal(ready.at[mz], inc=1, device_id=at(z, mx), device_id_type=MESH)

    @pl.when((mx == 0) & ~low)
    def _():
        pl.semaphore_signal(ready.at[mz], inc=1, device_id=at(0, 1), device_id_type=MESH)

    for x in range(nx - 1):
        @pl.when((x < mx) & ((x > 0) | ~low))
        def _():
            pl.semaphore_signal(x_ready.at[mx], inc=1, device_id=at(mz, x), device_id_type=MESH)

    small = [
        pltpu.make_async_copy(slot_hbm, slot, small_sem.at[0]),
        pltpu.make_async_copy(len_hbm, lens, small_sem.at[1]),
    ]
    loads = [pltpu.make_async_copy(k_hbm.at[s], kbuf.at[s], ksem) for s in range(slots)]
    vloads = [pltpu.make_async_copy(v_hbm.at[s], vbuf.at[s], vsem) for s in range(slots)]
    for c in small + loads + vloads:
        c.start()
    own.wait()
    first_row = q_land.at[0, 0]

    def row_copy(row, z, x, send, recv):
        return pltpu.make_async_remote_copy(
            src_ref=row, dst_ref=row, send_sem=send, recv_sem=recv, device_id=at(z, x), device_id_type=MESH)

    for x in range(nx):
        @pl.when((x > mx) & ~root)
        def _():
            pl.semaphore_wait(x_ready.at[x], 1)

        @pl.when((x != mx) & ((x > 0) | ~low) & ~root)
        def _():
            row_copy(q_land.at[mz, mx], mz, x, x_send_sem, x_recv_sem).start()

        @pl.when((x > 0) & root)
        def _():
            row_copy(first_row, 0, x, x_send_sem, root_sem).start()

    three = q_land.at[mz, pl.ds(0, nx - 1)]
    two = q_land.at[mz, pl.ds(0, nx - 2)]

    def piece(b):
        return q_land.at[0, pl.ds(1, nx - 1)] if isinstance(b, int) and b == 0 else q_land.at[b]

    def block_copy(b, z, x, sem):
        return row_copy(piece(b), z, x, sem, block_sem.at[b])

    def block_wait(b):
        pltpu.make_async_copy(piece(b), piece(b), block_sem.at[b]).wait()

    q_use[0, 0] = jnp.zeros((group, hd), BF16)

    @pl.when(low & ~root)
    def _():
        pltpu.make_async_copy(two, two, x_recv_sem).wait()

    @pl.when(~low)
    def _():
        pltpu.make_async_copy(three, three, x_recv_sem).wait()
        q_use[mz] = q_land[mz]

    for b in range(top_z):
        @pl.when((b < mz) & ((mx > 0) | (b > 0)))
        def _():
            block_copy(mz, b, mx, block_send).start()

    def send_row(z):
        @pl.when(low & ~root)
        def _():
            row_copy(first_row, z, mx, row_send, root_sem).start()

        @pl.when(agent)
        def _():
            row_copy(first_row, z, 0, row_send, root_sem).start()

    for z in range(1, nz):
        if z == middle:
            @pl.when(low & ~root)
            def _():
                pltpu.make_async_copy(first_row, first_row, root_sem).wait()

        @pl.when((z > mz) & ~root)
        def _():
            pl.semaphore_wait(ready.at[z], 1 + agent.astype(jnp.int32))

            @pl.when(~low)
            def _():
                block_copy(mz, z, mx, block_send).start()

            @pl.when(low)
            def _():
                block_copy(0, z, mx, block_send).start()

        @pl.when(agent)
        def _():
            block_copy(0, z, 0, col_send).start()

        if z >= middle:
            send_row(z)

    for z in range(1, middle):
        send_row(z)

    @pl.when(agent)
    def _():
        block_copy(0, 0, 0, root_send).start()

    for c in small:
        c.wait()
    per_seq = slots * n // nz
    code = [slot[s] for s in range(slots)]
    seq = [c // per_seq for c in code]
    col = lax.broadcasted_iota(jnp.int32, (1, slots * rows), 1)
    seq_at = jnp.zeros_like(col)
    for s in range(slots):
        seq_at = jnp.where(col // rows == s, seq[s], seq_at)
    r = lax.broadcasted_iota(jnp.int32, (nz * rows, slots * rows), 0)
    c = lax.broadcasted_iota(jnp.int32, (nz * rows, slots * rows), 1)
    wanted = r // (nz * group) * group + lax.rem(r, group)
    same = (lax.rem(r, nz * group) // group == seq_at) & (wanted == lax.rem(c, rows))
    gather[...] = jnp.where(same, 1.0, 0.0).astype(BF16)
    lane_slot = lax.broadcasted_iota(jnp.int32, (1, hd), 1)
    lane_seq = jnp.full((1, hd), -1, jnp.int32)
    lane_lead = jnp.zeros((1, hd), jnp.int32)
    for s in range(slots):
        lead = 1
        for t in range(s):
            lead = lead * (seq[t] != seq[s]).astype(jnp.int32)
        lane_seq = jnp.where(lax.rem(lane_slot, slots) == s, seq[s], lane_seq)
        lane_lead = jnp.where(lane_slot == s, lead, lane_lead)
    lane_seq = jnp.where(lane_slot < 3 * slots, lane_seq, -1)
    r = lax.broadcasted_iota(jnp.int32, (nz, hd), 0)
    gather_stat[...] = jnp.where(r == lane_seq, 1.0, 0.0).astype(BF16)

    pltpu.make_async_copy(k_hbm, kbuf, ksem).wait()
    for s in range(slots):
        for p in range(pairs):
            ktr[s, p] = kbuf[s, :, p].reshape(wide, hd).T
    pltpu.make_async_copy(v_hbm, vbuf, vsem).wait()

    row_pass = (mz < reach).astype(jnp.int32)

    def first(b):
        d = jnp.abs(mz - b)
        near = (mz <= middle) | (b < reach) | (jnp.minimum(d, nz - d) <= reach + 1)
        return ((b <= mz) & (mz >= reach) & near).astype(jnp.int32)

    def made(b, x):
        return row_pass if b == 0 and x == 0 else 1 - first(b)

    def goes(b, x, late):
        return late == (made(b, x) if b < reach else jnp.where(mz >= middle, 1, made(b, x)))

    scale = hd ** -0.5 * math.log2(math.e)

    def one_pass(late, carry):
        for b in range(nz):
            @pl.when((first(b) != late) & ((b != mz) | root))
            def _():
                block_wait(b)

            if b > 0:
                @pl.when(agent)
                def _():
                    block_copy(b, 0, 0, root_send).start()

                @pl.when((first(b) != late) & (b != mz))
                def _():
                    q_use[b] = q_land[b]
            else:
                @pl.when(first(b) != late)
                def _():
                    q_use[0, pl.ds(1, nx - 1)] = q_land[0, pl.ds(1, nx - 1)]

        @pl.when(late == row_pass)
        def _():
            @pl.when(~low)
            def _():
                pltpu.make_async_copy(first_row, first_row, root_sem).wait()

            q_use[0, 0] = q_land[0, 0]

        lane = lax.broadcasted_iota(jnp.int32, (rows, wide), 1)
        row = lax.broadcasted_iota(jnp.int32, (rows, wide), 0)
        matched = lax.rem(lane, half) == row // group
        token = jnp.where(matched, lane // half, block)
        left = []
        for b, c in zip(seq, code):
            rest = jnp.clip(lens[b] - lax.rem(c, per_seq) * block, 0, block)
            ours = (first(b) != late) | ((b == 0) & (late == row_pass))
            left.append(jnp.where(ours, rest, 0))
        work = [(p, s) for p in range(pairs) for s in range(slots)]

        def score(p, s):
            q = q_use[seq[s], pl.ds(p * half, half)].reshape(rows, hd)
            return jnp.dot(q, ktr[s, p], preferred_element_type=F32)

        def soften(sc, s):
            live = token < left[s]
            sc = jnp.where(live, sc, NEG)
            m = jnp.max(sc, axis=1, keepdims=True)
            w = jnp.where(live, jnp.exp2((sc - m) * scale), 0.0).astype(BF16)
            return m, jnp.sum(w.astype(F32), axis=1, keepdims=True), w

        peaks, totals, weights, parts = {}, {}, {}, {}
        scores = {}
        for i in range(len(work) + 2):
            if i < len(work):
                scores[i] = score(*work[i])
            if 0 <= i - 1 < len(work):
                peaks[i - 1], totals[i - 1], weights[i - 1] = soften(scores.pop(i - 1), work[i - 1][1])
            if i >= 2:
                p, s = work[i - 2]
                parts[i - 2] = jnp.dot(
                    weights.pop(i - 2), vbuf[s, :, p].reshape(wide, hd), preferred_element_type=F32)
        for p in range(pairs):
            peak, total, part = ([d[p * slots + s] for s in range(slots)] for d in (peaks, totals, parts))
            lane_s = lax.broadcasted_iota(jnp.int32, (rows, hd), 1)
            tops = jnp.full((rows, hd), NEG, F32)
            sums = jnp.zeros((rows, hd), F32)
            best = jnp.full((rows, hd), NEG, F32)
            for s in range(slots):
                tops = jnp.where(lane_s == s, peak[s], tops)
                sums = jnp.where(lane_s == s, total[s], sums)
                best = jnp.maximum(best, jnp.where(lane_seq == seq[s], peak[s], NEG))
            f = jnp.exp2((tops - best) * scale)
            sums = sums * f
            lead = jnp.where(lane_lead == 1, best, 0.0)
            both = jnp.concatenate([part[s] * f[:, s:s + 1] for s in range(slots)], axis=0).astype(BF16)
            acc = jnp.dot(gather[...], both, preferred_element_type=F32)
            for e in range(half):
                half_acc = acc[e * nz * group:(e + 1) * nz * group].reshape(nz, group, hd)
                out_send[late, p * half + e] = half_acc.astype(BF16)
            mixed = []
            for e in range(half):
                mixed += [lead[e * group:(e + 1) * group], sums[e * group:(e + 1) * group]]
            rest = jnp.concatenate(mixed + [jnp.zeros((hd - 2 * rows, hd), F32)], axis=0)
            packed = jnp.zeros((hd, hd), F32)
            for k in range(3):
                coarse = rest.astype(BF16).astype(F32)
                packed = packed + (pltpu.roll(coarse, k * slots, 1) if k else coarse)
                rest = rest - coarse
            st = lax.dot_general(
                gather_stat[...], packed.astype(BF16), (((1,), (1,)), ((), ())), preferred_element_type=F32)
            st_send[late, p] = st.reshape(nz, 1, hd)
        for b in range(nz):
            for x in range(nx):
                @pl.when(goes(b, x, late) & (b * nx + x != me))
                def _():
                    pltpu.make_async_remote_copy(
                        src_ref=out_send.at[made(b, x), x, b], dst_ref=out_recv.at[me],
                        send_sem=o_send_sem, recv_sem=o_recv_sem,
                        device_id=at(b, x), device_id_type=MESH).start()
                    pltpu.make_async_remote_copy(
                        src_ref=st_send.at[made(b, x), x // half, b], dst_ref=st_recv.at[me],
                        send_sem=s_send_sem, recv_sem=s_recv_sem,
                        device_id=at(b, x), device_id_type=MESH).start()
        return carry

    lax.fori_loop((mz < reach).astype(jnp.int32), 2, one_pass, 0)
    last = (mz < reach).astype(jnp.int32)
    out_recv[me] = out_send[last, mx, mz]
    st_recv[me] = st_send[last, mx // half, mz]
    rest_s = st_recv.at[pl.ds(0, n - 1)]
    rest_o = out_recv.at[pl.ds(0, n - 1)]
    @pl.when(low & ~root)
    def _():
        pltpu.make_async_copy(two, two, x_send_sem).wait()

    @pl.when(root | ~low)
    def _():
        pltpu.make_async_copy(three, three, x_send_sem).wait()

    def sent(sem, count):
        moved = out_recv.at[pl.ds(0, count)]
        pltpu.make_async_copy(moved, moved, sem).wait()

    @pl.when(~low & (mx > 0))
    def _():
        sent(block_send, (nz - 1) * nx)

    @pl.when(~low & (mx == 0))
    def _():
        sent(block_send, (nz - 2) * nx)

    @pl.when(low & ~root)
    def _():
        sent(block_send, (nz - 1) * (nx - 1))

    @pl.when(low & ~root & ~agent)
    def _():
        sent(row_send, nz - 1)

    @pl.when(agent)
    def _():
        sent(row_send, 2 * (nz - 1))
        sent(col_send, (nz - 1) * (nx - 1))
        sent(root_send, n - 1)

    pltpu.make_async_copy(rest_o, rest_o, o_send_sem).wait()
    pltpu.make_async_copy(rest_s, rest_s, s_send_sem).wait()
    pltpu.make_async_copy(rest_s, rest_s, s_recv_sem).wait()
    pltpu.make_async_copy(rest_o, rest_o, o_recv_sem).wait()

    stat = st_recv[...].reshape(n, hd)
    stat = jnp.where(lax.rem(mx, half) == 1, pltpu.roll(stat, hd - 2 * group, 1), stat)
    total = pltpu.roll(stat, hd - group, 1)
    stat = jnp.where(total > 0.0, stat, NEG)
    best = jnp.max(stat, axis=0, keepdims=True)
    f = jnp.exp2((stat - best) * scale)
    f = f / jnp.sum(f * total, axis=0, keepdims=True)
    r = lax.broadcasted_iota(jnp.int32, (group, hd), 0)
    c = lax.broadcasted_iota(jnp.int32, (group, hd), 1)
    acc = jnp.zeros((group, hd), F32)
    for i in range(n):
        g = jnp.where(c == r, jnp.broadcast_to(f[i:i + 1], (group, hd)), 0.0)
        acc = acc + jnp.sum(g, axis=1, keepdims=True) * out_recv[i].astype(F32)
    final[...] = acc.astype(BF16)
    out = pltpu.make_async_copy(final, o_hbm, small_sem.at[2])
    out.start()
    out.wait()


def solution(mesh):
    n = mesh.shape["seq"]

    def body(queries, keys, values, lengths, slot_block):
        share, _, hd = queries.shape
        slots, block, kv_local, _ = keys.shape
        nz = lengths.shape[0]
        nx = n // nz
        half = 2
        group = share
        split = (slots, block, nx // half, half, hd)
        any_ = pl.BlockSpec(memory_space=pl.ANY)
        dims = (nz, nx, slots, block, group, hd)
        dma, regular = pltpu.SemaphoreType.DMA, pltpu.SemaphoreType.REGULAR
        out = pl.pallas_call(
            functools.partial(attend, dims),
            out_shape=jax.ShapeDtypeStruct((share, hd), BF16),
            in_specs=[any_] * 5,
            out_specs=any_,
            scratch_shapes=[
                pltpu.VMEM(split, BF16), pltpu.VMEM(split, BF16),
                pltpu.VMEM((slots, nx // half, hd, block * half), BF16),
                pltpu.VMEM((nz * half * share, slots * half * share), BF16),
                pltpu.VMEM((nz, hd), BF16), pltpu.VMEM((share, hd), BF16),
                pltpu.VMEM((nz, nx, share, hd), BF16), pltpu.VMEM((nz, nx, share, hd), BF16),
                pltpu.SMEM((nz,), jnp.int32), pltpu.SMEM((slots,), jnp.int32),
                pltpu.VMEM((2, nx, nz, share, hd), BF16), pltpu.VMEM((n, share, hd), BF16),
                pltpu.VMEM((2, nx // half, nz, 1, hd), F32), pltpu.VMEM((n, 1, hd), F32),
                dma, dma, dma((3,)), regular((nz,)), regular((nx,)), dma, dma, dma, dma,
                dma, dma, dma, dma((nz,)), dma, dma, dma, dma,
            ],
            compiler_params=pltpu.CompilerParams(collective_id=0, has_side_effects=True),
        )(queries.reshape(share, hd), keys.reshape(split), values.reshape(split), lengths, slot_block)
        return out.reshape(share, 1, hd)

    placed = (
        P(("grp", "seq"), "head", None),
        P(("grp", "seq"), None, "head", None),
        P(("grp", "seq"), None, "head", None),
        P("grp"),
        P(("grp", "seq")),
    )
    return jax.shard_map(
        body, mesh=mesh, in_specs=placed, out_specs=P(("grp", "seq"), "head", None), check_vma=False
    )
```

```python
import functools
import math

import jax
import jax.numpy as jnp
from jax import lax
from jax.experimental import pallas as pl
from jax.experimental.pallas import tpu as pltpu
from jax.sharding import PartitionSpec as P

MESH = pl.DeviceIdType.MESH
F32 = jnp.float32
BF16 = jnp.bfloat16
NEG = -1e30


def attend(dims, q_hbm, k_hbm, v_hbm, len_hbm, slot_hbm, o_hbm,
           kbuf, vbuf, ktr, gather, gather_stat, final, q_land, q_use, lens, slot, out_send, out_recv, st_send, st_recv,
           ksem, vsem, small_sem, ready, x_ready, root_sem, row_send, root_send, col_send, x_send_sem, x_recv_sem, block_send, block_sem,
           o_send_sem, o_recv_sem, s_send_sem, s_recv_sem):
    nz, nx, slots, block, group, hd = dims
    n = nz * nx
    half = 2
    pairs = nx // half
    rows = half * group
    wide = block * half
    me = lax.axis_index("seq")
    mz, mx = me // nx, lax.rem(me, nx)
    top_z = nz - 1

    reach = nz // 4
    middle = nz // 2

    def at(z, x):
        return {"seq": z * nx + x}

    low = mz == 0
    root = me == 0
    agent = me == 1

    barrier = pltpu.get_barrier_semaphore()

    def greet(z, x):
        pl.semaphore_signal(barrier, inc=1, device_id=at(z, x), device_id_type=MESH)

    for z in range(top_z, 0, -1):
        @pl.when((z > mz) & ~root)
        def _():
            greet(z, mx)

        @pl.when(agent)
        def _():
            greet(z, 0)

    for x in range(nx):
        @pl.when(((x > mx) & ~root) | ((x == 0) & low & ~root))
        def _():
            greet(mz, x)

    own = pltpu.make_async_copy(q_hbm, q_land.at[mz, mx], small_sem.at[2])
    own.start()

    @pl.when(root)
    def _():
        pl.semaphore_wait(barrier, nx - 1)

    @pl.when(me > 1)
    def _():
        pl.semaphore_wait(barrier, mz + mx - low.astype(jnp.int32))

    for z in range(top_z):
        @pl.when((z < mz) & ((mx > 0) | (z > 0)))
        def _():
            pl.semaphore_signal(ready.at[mz], inc=1, device_id=at(z, mx), device_id_type=MESH)

    @pl.when((mx == 0) & ~low)
    def _():
        pl.semaphore_signal(ready.at[mz], inc=1, device_id=at(0, 1), device_id_type=MESH)

    for x in range(nx - 1):
        @pl.when((x < mx) & ((x > 0) | ~low))
        def _():
            pl.semaphore_signal(x_ready.at[mx], inc=1, device_id=at(mz, x), device_id_type=MESH)

    small = [
        pltpu.make_async_copy(slot_hbm, slot, small_sem.at[0]),
        pltpu.make_async_copy(len_hbm, lens, small_sem.at[1]),
    ]
    loads = [pltpu.make_async_copy(k_hbm.at[s], kbuf.at[s], ksem) for s in range(slots)]
    vloads = [pltpu.make_async_copy(v_hbm.at[s], vbuf.at[s], vsem) for s in range(slots)]
    for c in small + loads + vloads:
        c.start()
    own.wait()
    first_row = q_land.at[0, 0]

    def row_copy(row, z, x, send, recv):
        return pltpu.make_async_remote_copy(
            src_ref=row, dst_ref=row, send_sem=send, recv_sem=recv, device_id=at(z, x), device_id_type=MESH)

    for x in range(nx):
        @pl.when((x > mx) & ~root)
        def _():
            pl.semaphore_wait(x_ready.at[x], 1)

        @pl.when((x != mx) & ((x > 0) | ~low) & ~root)
        def _():
            row_copy(q_land.at[mz, mx], mz, x, x_send_sem, x_recv_sem).start()

        @pl.when((x > 0) & root)
        def _():
            row_copy(first_row, 0, x, x_send_sem, root_sem).start()

    three = q_land.at[mz, pl.ds(0, nx - 1)]
    two = q_land.at[mz, pl.ds(0, nx - 2)]

    def piece(b):
        return q_land.at[0, pl.ds(1, nx - 1)] if isinstance(b, int) and b == 0 else q_land.at[b]

    def block_copy(b, z, x, sem):
        return row_copy(piece(b), z, x, sem, block_sem.at[b])

    def block_wait(b):
        pltpu.make_async_copy(piece(b), piece(b), block_sem.at[b]).wait()

    q_use[0, 0] = jnp.zeros((group, hd), BF16)

    @pl.when(low & ~root)
    def _():
        pltpu.make_async_copy(two, two, x_recv_sem).wait()

    @pl.when(~low)
    def _():
        pltpu.make_async_copy(three, three, x_recv_sem).wait()
        q_use[mz] = q_land[mz]

    for b in range(top_z):
        @pl.when((b < mz) & ((mx > 0) | (b > 0)))
        def _():
            block_copy(mz, b, mx, block_send).start()

    def send_row(z):
        @pl.when(low & ~root)
        def _():
            row_copy(first_row, z, mx, row_send, root_sem).start()

        @pl.when(agent)
        def _():
            row_copy(first_row, z, 0, row_send, root_sem).start()

    for z in range(1, nz):
        if z == middle:
            @pl.when(low & ~root)
            def _():
                pltpu.make_async_copy(first_row, first_row, root_sem).wait()

        @pl.when((z > mz) & ~root)
        def _():
            pl.semaphore_wait(ready.at[z], 1 + agent.astype(jnp.int32))

            @pl.when(~low)
            def _():
                block_copy(mz, z, mx, block_send).start()

            @pl.when(low)
            def _():
                block_copy(0, z, mx, block_send).start()

        @pl.when(agent)
        def _():
            block_copy(0, z, 0, col_send).start()

        if z >= middle:
            send_row(z)

    for z in range(1, middle):
        send_row(z)

    @pl.when(agent)
    def _():
        block_copy(0, 0, 0, root_send).start()

    for c in small:
        c.wait()
    per_seq = slots * n // nz
    code = [slot[s] for s in range(slots)]
    seq = [c // per_seq for c in code]
    col = lax.broadcasted_iota(jnp.int32, (1, slots * rows), 1)
    seq_at = jnp.zeros_like(col)
    for s in range(slots):
        seq_at = jnp.where(col // rows == s, seq[s], seq_at)
    r = lax.broadcasted_iota(jnp.int32, (nz * rows, slots * rows), 0)
    c = lax.broadcasted_iota(jnp.int32, (nz * rows, slots * rows), 1)
    wanted = r // (nz * group) * group + lax.rem(r, group)
    same = (lax.rem(r, nz * group) // group == seq_at) & (wanted == lax.rem(c, rows))
    gather[...] = jnp.where(same, 1.0, 0.0).astype(BF16)
    lane_slot = lax.broadcasted_iota(jnp.int32, (1, hd), 1)
    lane_seq = jnp.full((1, hd), -1, jnp.int32)
    lane_lead = jnp.zeros((1, hd), jnp.int32)
    for s in range(slots):
        lead = 1
        for t in range(s):
            lead = lead * (seq[t] != seq[s]).astype(jnp.int32)
        lane_seq = jnp.where(lax.rem(lane_slot, slots) == s, seq[s], lane_seq)
        lane_lead = jnp.where(lane_slot == s, lead, lane_lead)
    lane_seq = jnp.where(lane_slot < 3 * slots, lane_seq, -1)
    r = lax.broadcasted_iota(jnp.int32, (nz, hd), 0)
    gather_stat[...] = jnp.where(r == lane_seq, 1.0, 0.0).astype(BF16)

    pltpu.make_async_copy(k_hbm, kbuf, ksem).wait()
    for s in range(slots):
        for p in range(pairs):
            ktr[s, p] = kbuf[s, :, p].reshape(wide, hd).T
    pltpu.make_async_copy(v_hbm, vbuf, vsem).wait()

    row_pass = (mz < reach).astype(jnp.int32)

    def first(b):
        d = jnp.abs(mz - b)
        near = (mz <= middle) | (b < reach) | (jnp.minimum(d, nz - d) <= reach + 1)
        return ((b <= mz) & (mz >= reach) & near).astype(jnp.int32)

    def goes(b, x, late):
        return late == row_pass if b == 0 and x == 0 else first(b) != late

    scale = hd ** -0.5 * math.log2(math.e)

    def one_pass(late, carry):
        for b in range(nz):
            @pl.when((first(b) != late) & ((b != mz) | root))
            def _():
                block_wait(b)

            if b > 0:
                @pl.when(agent)
                def _():
                    block_copy(b, 0, 0, root_send).start()

                @pl.when((first(b) != late) & (b != mz))
                def _():
                    q_use[b] = q_land[b]
            else:
                @pl.when(first(b) != late)
                def _():
                    q_use[0, pl.ds(1, nx - 1)] = q_land[0, pl.ds(1, nx - 1)]

        @pl.when(late == row_pass)
        def _():
            @pl.when(~low)
            def _():
                pltpu.make_async_copy(first_row, first_row, root_sem).wait()

            q_use[0, 0] = q_land[0, 0]

        lane = lax.broadcasted_iota(jnp.int32, (rows, wide), 1)
        row = lax.broadcasted_iota(jnp.int32, (rows, wide), 0)
        matched = lax.rem(lane, half) == row // group
        token = jnp.where(matched, lane // half, block)
        left = []
        for b, c in zip(seq, code):
            rest = jnp.clip(lens[b] - lax.rem(c, per_seq) * block, 0, block)
            ours = (first(b) != late) | ((b == 0) & (late == row_pass))
            left.append(jnp.where(ours, rest, 0))
        work = [(p, s) for p in range(pairs) for s in range(slots)]

        def score(p, s):
            q = q_use[seq[s], pl.ds(p * half, half)].reshape(rows, hd)
            return jnp.dot(q, ktr[s, p], preferred_element_type=F32)

        def soften(sc, s):
            live = token < left[s]
            sc = jnp.where(live, sc, NEG)
            m = jnp.max(sc, axis=1, keepdims=True)
            w = jnp.where(live, jnp.exp2((sc - m) * scale), 0.0).astype(BF16)
            return m, jnp.sum(w.astype(F32), axis=1, keepdims=True), w

        peaks, totals, weights, parts = {}, {}, {}, {}
        scores = {}
        for i in range(len(work) + 2):
            if i < len(work):
                scores[i] = score(*work[i])
            if 0 <= i - 1 < len(work):
                peaks[i - 1], totals[i - 1], weights[i - 1] = soften(scores.pop(i - 1), work[i - 1][1])
            if i >= 2:
                p, s = work[i - 2]
                parts[i - 2] = jnp.dot(
                    weights.pop(i - 2), vbuf[s, :, p].reshape(wide, hd), preferred_element_type=F32)
        for p in range(pairs):
            peak, total, part = ([d[p * slots + s] for s in range(slots)] for d in (peaks, totals, parts))
            lane_s = lax.broadcasted_iota(jnp.int32, (rows, hd), 1)
            tops = jnp.full((rows, hd), NEG, F32)
            sums = jnp.zeros((rows, hd), F32)
            best = jnp.full((rows, hd), NEG, F32)
            for s in range(slots):
                tops = jnp.where(lane_s == s, peak[s], tops)
                sums = jnp.where(lane_s == s, total[s], sums)
                best = jnp.maximum(best, jnp.where(lane_seq == seq[s], peak[s], NEG))
            f = jnp.exp2((tops - best) * scale)
            sums = sums * f
            lead = jnp.where(lane_lead == 1, best, 0.0)
            both = jnp.concatenate([part[s] * f[:, s:s + 1] for s in range(slots)], axis=0).astype(BF16)
            acc = jnp.dot(gather[...], both, preferred_element_type=F32)
            for e in range(half):
                half_acc = acc[e * nz * group:(e + 1) * nz * group].reshape(nz, group, hd)
                out_send[late, p * half + e] = half_acc.astype(BF16)
            mixed = []
            for e in range(half):
                mixed += [lead[e * group:(e + 1) * group], sums[e * group:(e + 1) * group]]
            rest = jnp.concatenate(mixed + [jnp.zeros((hd - 2 * rows, hd), F32)], axis=0)
            packed = jnp.zeros((hd, hd), F32)
            for k in range(3):
                coarse = rest.astype(BF16).astype(F32)
                packed = packed + (pltpu.roll(coarse, k * slots, 1) if k else coarse)
                rest = rest - coarse
            st = lax.dot_general(
                gather_stat[...], packed.astype(BF16), (((1,), (1,)), ((), ())), preferred_element_type=F32)
            st_send[late, p] = st.reshape(nz, 1, hd)
        for b in range(nz):
            for x in range(nx):
                @pl.when(goes(b, x, late) & (b * nx + x != me))
                def _():
                    pltpu.make_async_remote_copy(
                        src_ref=out_send.at[late, x, b], dst_ref=out_recv.at[me],
                        send_sem=o_send_sem, recv_sem=o_recv_sem,
                        device_id=at(b, x), device_id_type=MESH).start()
                    pltpu.make_async_remote_copy(
                        src_ref=st_send.at[late, x // half, b], dst_ref=st_recv.at[me],
                        send_sem=s_send_sem, recv_sem=s_recv_sem,
                        device_id=at(b, x), device_id_type=MESH).start()
        return carry

    lax.fori_loop((mz < reach).astype(jnp.int32), 2, one_pass, 0)
    last = (mz < reach).astype(jnp.int32)
    out_recv[me] = out_send[last, mx, mz]
    st_recv[me] = st_send[last, mx // half, mz]
    rest_s = st_recv.at[pl.ds(0, n - 1)]
    rest_o = out_recv.at[pl.ds(0, n - 1)]
    @pl.when(low & ~root)
    def _():
        pltpu.make_async_copy(two, two, x_send_sem).wait()

    @pl.when(root | ~low)
    def _():
        pltpu.make_async_copy(three, three, x_send_sem).wait()

    def sent(sem, count):
        moved = out_recv.at[pl.ds(0, count)]
        pltpu.make_async_copy(moved, moved, sem).wait()

    @pl.when(~low & (mx > 0))
    def _():
        sent(block_send, (nz - 1) * nx)

    @pl.when(~low & (mx == 0))
    def _():
        sent(block_send, (nz - 2) * nx)

    @pl.when(low & ~root)
    def _():
        sent(block_send, (nz - 1) * (nx - 1))

    @pl.when(low & ~root & ~agent)
    def _():
        sent(row_send, nz - 1)

    @pl.when(agent)
    def _():
        sent(row_send, 2 * (nz - 1))
        sent(col_send, (nz - 1) * (nx - 1))
        sent(root_send, n - 1)

    pltpu.make_async_copy(rest_o, rest_o, o_send_sem).wait()
    pltpu.make_async_copy(rest_s, rest_s, s_send_sem).wait()
    pltpu.make_async_copy(rest_s, rest_s, s_recv_sem).wait()
    pltpu.make_async_copy(rest_o, rest_o, o_recv_sem).wait()

    stat = st_recv[...].reshape(n, hd)
    stat = jnp.where(lax.rem(mx, half) == 1, pltpu.roll(stat, hd - 2 * group, 1), stat)
    total = pltpu.roll(stat, hd - group, 1)
    stat = jnp.where(total > 0.0, stat, NEG)
    best = jnp.max(stat, axis=0, keepdims=True)
    f = jnp.exp2((stat - best) * scale)
    f = f / jnp.sum(f * total, axis=0, keepdims=True)
    r = lax.broadcasted_iota(jnp.int32, (group, hd), 0)
    c = lax.broadcasted_iota(jnp.int32, (group, hd), 1)
    acc = jnp.zeros((group, hd), F32)
    for i in range(n):
        g = jnp.where(c == r, jnp.broadcast_to(f[i:i + 1], (group, hd)), 0.0)
        acc = acc + jnp.sum(g, axis=1, keepdims=True) * out_recv[i].astype(F32)
    final[...] = acc.astype(BF16)
    out = pltpu.make_async_copy(final, o_hbm, small_sem.at[2])
    out.start()
    out.wait()


def solution(mesh):
    n = mesh.shape["seq"]

    def body(queries, keys, values, lengths, slot_block):
        share, _, hd = queries.shape
        slots, block, kv_local, _ = keys.shape
        nz = lengths.shape[0]
        nx = n // nz
        half = 2
        group = share
        split = (slots, block, nx // half, half, hd)
        any_ = pl.BlockSpec(memory_space=pl.ANY)
        dims = (nz, nx, slots, block, group, hd)
        dma, regular = pltpu.SemaphoreType.DMA, pltpu.SemaphoreType.REGULAR
        out = pl.pallas_call(
            functools.partial(attend, dims),
            out_shape=jax.ShapeDtypeStruct((share, hd), BF16),
            in_specs=[any_] * 5,
            out_specs=any_,
            scratch_shapes=[
                pltpu.VMEM(split, BF16), pltpu.VMEM(split, BF16),
                pltpu.VMEM((slots, nx // half, hd, block * half), BF16),
                pltpu.VMEM((nz * half * share, slots * half * share), BF16),
                pltpu.VMEM((nz, hd), BF16), pltpu.VMEM((share, hd), BF16),
                pltpu.VMEM((nz, nx, share, hd), BF16), pltpu.VMEM((nz, nx, share, hd), BF16),
                pltpu.SMEM((nz,), jnp.int32), pltpu.SMEM((slots,), jnp.int32),
                pltpu.VMEM((2, nx, nz, share, hd), BF16), pltpu.VMEM((n, share, hd), BF16),
                pltpu.VMEM((2, nx // half, nz, 1, hd), F32), pltpu.VMEM((n, 1, hd), F32),
                dma, dma, dma((3,)), regular((nz,)), regular((nx,)), dma, dma, dma, dma,
                dma, dma, dma, dma((nz,)), dma, dma, dma, dma,
            ],
            compiler_params=pltpu.CompilerParams(collective_id=0, has_side_effects=True),
        )(queries.reshape(share, hd), keys.reshape(split), values.reshape(split), lengths, slot_block)
        return out.reshape(share, 1, hd)

    placed = (
        P(("grp", "seq"), "head", None),
        P(("grp", "seq"), None, "head", None),
        P(("grp", "seq"), None, "head", None),
        P("grp"),
        P(("grp", "seq")),
    )
    return jax.shard_map(
        body, mesh=mesh, in_specs=placed, out_specs=P(("grp", "seq"), "head", None), check_vma=False
    )
```
